768 devices in a mesh: dp: 64 (over x, y, core), tensor: 12 (over z).
Axes of the slice: x: 4, y: 8, z: 12, core: 2. Of those that a mesh axis runs over, the one named last changes fastest.
Arguments:
- gradient: float32 [5120, 27648], P('dp', 'tensor'), may hold values from -6 to 6
- momentum: float32 [5120, 27648], P('dp', 'tensor'), may hold values from -6 to 6
- right_factor: float32 [27648, 256], P('tensor'), may hold values from -6 to 6
Outputs:
- update: float32 [5120, 27648], P('dp', 'tensor')
- new_momentum: float32 [5120, 27648], P('dp', 'tensor')
- new_right: float32 [27648, 256], P('tensor')
The draws below stay inside these ranges and needn't reach their ends.
All inputs are finite; a program needn't handle non-finite values.
Results may differ from the reference program's by a relative error of at most 0.000098.
Values sent between devices are 32-bit elements; how exact they have to be, the bound alone decides.
A program may use at most 64 MiB of HBM per device.

```python
import jax
import jax.numpy as jnp
from jax import lax

ROWS = 5120
COLS = 27648
RANK = 256


def shard_levels(key, dims, cuts, least, largest):
    def one(axis_at, shards_of):
        heights = jax.random.uniform(jax.random.fold_in(jax.random.fold_in(key, 6), axis_at), (shards_of,), jnp.float32, least / len(cuts), largest / len(cuts))
        return jnp.repeat(jnp.exp(heights), dims[axis_at] // shards_of).reshape((-1,) + (1,) * (len(dims) - axis_at - 1))

    loudness = one(*cuts[0])
    for cut in cuts[1:]:
        loudness = loudness * one(*cut)
    return loudness


def centred(rng, shape, scale, limit, split=(), dtype=jnp.bfloat16):
    array = jax.random.normal(rng, shape, jnp.float32) * scale
    if len(split) > 0:
        array = shard_levels(rng, shape, split, -0.22, 0.18) * array
    return jnp.clip(array, min=-limit, max=limit).astype(dtype)


def setup_inputs(seed: int = 0) -> dict:
    seeds = jax.random.split(jax.random.key(seed), 4)
    return {
        "gradient": centred(seeds[0], (ROWS, COLS), 1.0, 6.0, ((0, 64), (1, 12)), jnp.float32),
        "momentum": centred(seeds[1], (ROWS, COLS), 1.0, 6.0, ((0, 64), (1, 12)), jnp.float32),
        "right_factor": centred(seeds[2], (COLS, RANK), 1.0, 6.0, ((0, 12),), jnp.float32),
    }


def reference(gradient, momentum, right_factor):
    high = lax.Precision.HIGHEST
    buffer = momentum + gradient
    left = jnp.dot(buffer.astype(jnp.float32), right_factor.astype(jnp.float32), precision=high, preferred_element_type=jnp.float32)
    gram = jnp.dot(left.T.astype(jnp.float32), left.astype(jnp.float32), precision=high, preferred_element_type=jnp.float32)
    chol = jnp.linalg.cholesky(gram)
    ortho = jax.scipy.linalg.solve_triangular(chol, left.T, lower=True).T
    right = jnp.dot(buffer.T.astype(jnp.float32), ortho.astype(jnp.float32), precision=high, preferred_element_type=jnp.float32)
    scale_col = jnp.sqrt(lax.optimization_barrier(jnp.sum(right * right, axis=0)) / COLS + 1e-06)
    new_right = right / scale_col
    new_momentum = buffer - 0.05 * jnp.dot(ortho.astype(jnp.float32), right.T.astype(jnp.float32), precision=high, preferred_element_type=jnp.float32)
    factor = (ROWS / RANK) ** 0.5
    update = factor * jnp.dot(ortho.astype(jnp.float32), new_right.T.astype(jnp.float32), precision=high, preferred_element_type=jnp.float32)
    return (update, new_momentum, new_right)
```

```python
import jax
import jax.numpy as jnp
from jax import lax
from jax.experimental import pallas as pl
from jax.experimental.pallas import tpu as pltpu
from jax.sharding import Mesh
from jax.sharding import PartitionSpec as P

ROWS = 5120
COLS = 27648
RANK = 256
NX, NY, NC, NZ = 4, 8, 2, 12
DP = ("dp_0", "dp_1", "dp_2")
HIGH = lax.Precision.HIGHEST
F32 = jnp.float32
MESH = pl.DeviceIdType.MESH
LOCAL_ROWS = ROWS // (NX * NY * NC)
LOCAL_COLS = COLS // NZ
BLOCKS = LOCAL_COLS // 256
X_FIRST = 6
Y_FIRST = BLOCKS - X_FIRST
XW, YW = 128 * X_FIRST, 128 * Y_FIRST
PANEL = 64


def dot(a, b, dims=((1,), (0,))):
    return lax.dot_general(a, b, (dims, ((), ())), precision=HIGH, preferred_element_type=F32)


def eliminate_slab(ws, p, s):
    r0 = PANEL * p + 8 * s
    end = PANEL * (p + 1)
    n = end - r0
    lo = (r0 // 128) * 128
    hi = RANK + (r0 // 128 + 1) * 128
    cols = [jnp.broadcast_to(ws[r0:end, r0 + j : r0 + j + 1], (n, 128)) for j in range(8)]
    w = ws[r0:end, lo:hi]
    sub = lax.broadcasted_iota(jnp.int32, (n, 128), 0)
    wide_sub = lax.broadcasted_iota(jnp.int32, w.shape, 0)
    reps = (hi - lo) // 128
    for j in range(8):
        rs = lax.rsqrt(cols[j][j : j + 1, :])
        l = cols[j] * rs
        for m in range(j + 1, 8):
            cols[m] = cols[m] - l * l[m : m + 1, :]
        lm = jnp.concatenate([jnp.where(sub > j, l, 0.0)] * reps, axis=1)
        u = w[j : j + 1, :] * jnp.concatenate([rs] * reps, axis=1)
        w = jnp.where(wide_sub == j, jnp.broadcast_to(u, w.shape), w - lm * u)
    ws[r0:end, lo:hi] = w


def update_below(ws, p):
    a, b = PANEL * p, PANEL * (p + 1)
    lo = (b // 128) * 128
    hi = RANK + ((b - 1) // 128 + 1) * 128
    full = dot(ws[a:b, lo:RANK], ws[a:b, lo:hi], ((0,), (0,)))
    ws[b:RANK, lo:hi] = ws[b:RANK, lo:hi] - full[b - lo :, :]


def factor_panel(ws, p):
    for s in range(PANEL // 8):
        eliminate_slab(ws, p, s)
    if PANEL * (p + 1) < RANK:
        update_below(ws, p)


def offsets(n):
    return sorted(range(1, n), key=lambda off: -min(off, n - off))


def main_kernel(
    g_ref, m_ref, r_ref, rt_ref, ortho_ref, inv_ref,
    bbuf, pbuf, pin, lbuf, lt, gp, gpin, gyin, gxs, gfull, ws,
    mx, my, mxin, myin, xin1, xs, xin2, yin1, ys, yin2, fx, fy, sq,
    pa_s, pa_r, lb_s, lb_r, pr_s, pr_r, gy_s, gy_r, gx_s, gx_r, ga_s, ga_r, gd_s, gd_r,
    x1_s, x1_r, x2_s, x2_r, y1_s, y1_r, y2_s, y2_r,
    ax1_s, ax1_r, ax2_s, ax2_r, ay1_s, ay1_r, ay2_s, ay2_r, dd_s, dd_r, sq_s, sq_r,
):
    x, y, c, z = (lax.axis_index(a) for a in (*DP, "tensor"))
    other = 1 - c

    def at_x(off):
        return lax.rem(x + off, NX)

    def at_y(off):
        return lax.rem(y + off, NY)

    def at_z(off):
        return lax.rem(z + off, NZ)

    def send(src, dst, s, r, where):
        copy = pltpu.make_async_remote_copy(
            src_ref=src, dst_ref=dst, send_sem=s, recv_sem=r, device_id=where, device_id_type=MESH
        )
        copy.start()
        return copy

    barrier = pltpu.get_barrier_semaphore()
    greet = [{"tensor": at_z(o)} for o in range(1, NZ)]
    greet += [{"dp_1": at_y(o)} for o in range(1, NY)]
    greet += [{"dp_0": at_x(o)} for o in range(1, NX)]
    greet += [{"dp_2": other}]
    for where in greet:
        pl.semaphore_signal(barrier, inc=1, device_id=where, device_id_type=MESH)

    pending = []

    b = g_ref[...] + m_ref[...]
    bbuf[0:LOCAL_ROWS, :] = b
    bbuf[LOCAL_ROWS:128, :] = jnp.zeros((128 - LOCAL_ROWS, LOCAL_COLS), F32)
    part = dot(bbuf[0:LOCAL_ROWS, :], r_ref[...])
    for i in range(NZ):
        if 8 * i < LOCAL_ROWS:
            pbuf[i] = part[8 * i : 8 * i + 8, :]
        else:
            pbuf[i] = jnp.zeros((8, RANK), F32)
    pl.semaphore_wait(barrier, len(greet))

    copies = {}
    for o in offsets(NZ):
        to = at_z(o)
        copies[o] = send(pbuf.at[to], pin.at[o - 1], pa_s.at[o - 1], pa_r.at[o - 1], {"tensor": to})
    total = pbuf[z]
    for o in range(1, NZ):
        copies[o].wait_recv()
        total = total + pin[o - 1]
    pending += copies.values()
    lbuf[z] = total
    copies = {}
    for o in offsets(NZ):
        copies[o] = send(lbuf.at[z], lbuf.at[z], lb_s.at[o - 1], lb_r.at[o - 1], {"tensor": at_z(o)})
    for o in range(1, NZ):
        copies[o].wait_recv()
    pending += copies.values()

    left = jnp.concatenate([lbuf[i] for i in range(LOCAL_ROWS // 8)] + [jnp.zeros((128 - LOCAL_ROWS, RANK), F32)], axis=0)
    lt[...] = left.T

    gram = dot(lt[...], left)
    for h in range(NC):
        for i in range(NY):
            gp[h, i] = gram[128 * h + 16 * i : 128 * h + 16 * i + 16, :]
    pair = {"dp_2": other}
    g_pair = send(gp.at[other], gpin, pr_s.at[0], pr_r.at[0], pair)

    def products(h):
        rows = lt[pl.ds(pl.multiple_of(128 * h, 128), 128), :]
        for t in range(BLOCKS):
            d = dot(rows, bbuf[:, 256 * t : 256 * t + 256])
            for i in range(NY):
                for q in range(2):
                    for k in range(2):
                        piece = d[16 * i + 8 * q : 16 * i + 8 * q + 8, 128 * k : 128 * k + 128]
                        if t < X_FIRST:
                            mx[h, 2 * q + k, i, :, 128 * t : 128 * t + 128] = piece
                        else:
                            my[h, 2 * q + k, i, :, 128 * (t - X_FIRST) : 128 * (t - X_FIRST) + 128] = piece

    products(other)
    y_pair = send(my.at[other], myin, pr_s.at[1], pr_r.at[1], pair)
    x_pair = send(mx.at[other], mxin, pr_s.at[2], pr_r.at[2], pair)

    g_pair.wait_recv()
    for i in range(NY):
        gp[c, i] = gp[c, i] + gpin[i]
    copies_g = {}
    for o in offsets(NY):
        to = at_y(o)
        copies_g[o] = send(gp.at[c, to], gyin.at[o - 1], gy_s.at[o - 1], gy_r.at[o - 1], {"dp_1": to})

    products(c)
    y_pair.wait_recv()
    for i in range(NX):
        my[c, i] = my[c, i] + myin[i]
    copies_y1 = {}
    for o in offsets(NY):
        to = at_y(o)
        copies_y1[o] = send(my.at[c, :, to], yin1.at[o - 1], y1_s.at[o - 1], y1_r.at[o - 1], {"dp_1": to})
    x_pair.wait_recv()
    for i in range(NX):
        mx[c, i] = mx[c, i] + mxin[i]
    copies_x1 = {}
    for o in offsets(NX):
        to = at_x(o)
        copies_x1[o] = send(mx.at[c, to], xin1.at[o - 1], x1_s.at[o - 1], x1_r.at[o - 1], {"dp_0": to})
    pending += [g_pair, y_pair, x_pair, *copies_g.values(), *copies_y1.values(), *copies_x1.values()]

    total = gp[c, y]
    for o in range(1, NY):
        copies_g[o].wait_recv()
        total = total + gyin[o - 1]
    gxs[x] = total
    copies = {}
    for o in offsets(NX):
        copies[o] = send(gxs.at[x], gxs.at[x], gx_s.at[o - 1], gx_r.at[o - 1], {"dp_0": at_x(o)})
    pending += copies.values()

    for o in range(1, NY):
        copies_y1[o].wait_recv()
    for i in range(NX):
        acc = my[c, i, y]
        for o in range(1, NY):
            acc = acc + yin1[o - 1, i]
        ys[i] = acc
    copies_y2 = {}
    for o in offsets(NX):
        to = at_x(o)
        copies_y2[o] = send(ys.at[to], yin2.at[o - 1], y2_s.at[o - 1], y2_r.at[o - 1], {"dp_0": to})
    pending += copies_y2.values()

    for o in range(1, NX):
        copies[o].wait_recv()
    total = gxs[0]
    for i in range(1, NX):
        total = total + gxs[i]
    gfull[c, y] = total
    copies_ga = {}
    for o in offsets(NY):
        copies_ga[o] = send(gfull.at[c, y], gfull.at[c, y], ga_s.at[o - 1], ga_r.at[o - 1], {"dp_1": at_y(o)})
    pending += copies_ga.values()

    for o in range(1, NX):
        copies_x1[o].wait_recv()
    for i in range(NY):
        acc = mx[c, x, i]
        for o in range(1, NX):
            acc = acc + xin1[o - 1, i]
        xs[i] = acc
    copies_x2 = {}
    for o in offsets(NY):
        to = at_y(o)
        copies_x2[o] = send(xs.at[to], xin2.at[o - 1], x2_s.at[o - 1], x2_r.at[o - 1], {"dp_1": to})
    pending += copies_x2.values()

    for o in range(1, NY):
        copies_ga[o].wait_recv()
    g_both = send(gfull.at[c], gfull.at[c], gd_s, gd_r, pair)
    pending += [g_both]

    acc = ys[x]
    for o in range(1, NX):
        copies_y2[o].wait_recv()
        acc = acc + yin2[o - 1]
    fy[c, x, y] = acc
    back_y1 = {}
    for o in offsets(NX):
        back_y1[o] = send(fy.at[c, x, y], fy.at[c, x, y], ay1_s.at[o - 1], ay1_r.at[o - 1], {"dp_0": at_x(o)})
    pending += back_y1.values()

    g_both.wait_recv()
    for h in range(NC):
        for i in range(NY):
            r0 = 128 * h + 16 * i
            ws[r0 : r0 + 16, 0:RANK] = gfull[h, i]
    ri = lax.broadcasted_iota(jnp.int32, (RANK, RANK), 0)
    ci = lax.broadcasted_iota(jnp.int32, (RANK, RANK), 1)
    ws[:, RANK:] = jnp.where(ri == ci, 1.0, 0.0)

    acc = xs[y]
    for o in range(1, NY):
        copies_x2[o].wait_recv()
        acc = acc + xin2[o - 1]
    fx[c, x, y] = acc
    back_x1 = {}
    for o in offsets(NY):
        back_x1[o] = send(fx.at[c, x, y], fx.at[c, x, y], ax1_s.at[o - 1], ax1_r.at[o - 1], {"dp_1": at_y(o)})
    pending += back_x1.values()

    factor_panel(ws, 0)

    for o in range(1, NX):
        back_y1[o].wait_recv()
    back_y2 = {}
    for o in offsets(NY):
        back_y2[o] = send(fy.at[c, :, y], fy.at[c, :, y], ay2_s.at[o - 1], ay2_r.at[o - 1], {"dp_1": at_y(o)})
    pending += back_y2.values()

    factor_panel(ws, 1)

    for o in range(1, NY):
        back_x1[o].wait_recv()
    back_x2 = {}
    for o in offsets(NX):
        back_x2[o] = send(fx.at[c, x], fx.at[c, x], ax2_s.at[o - 1], ax2_r.at[o - 1], {"dp_0": at_x(o)})
    pending += back_x2.values()

    factor_panel(ws, 2)
    factor_panel(ws, 3)
    inverse = ws[:, RANK:]
    ortho_ref[...] = dot(left[0:LOCAL_ROWS, :], inverse, ((1,), (1,)))

    for o in range(1, NY):
        back_y2[o].wait_recv()
    y_both = send(fy.at[c], fy.at[c], dd_s.at[0], dd_r.at[0], pair)
    for o in range(1, NX):
        back_x2[o].wait_recv()
    x_both = send(fx.at[c], fx.at[c], dd_s.at[1], dd_r.at[1], pair)
    pending += [y_both, x_both]
    y_both.wait_recv()
    x_both.wait_recv()

    inverse = ws[:, RANK:]
    acc = jnp.zeros((RANK, 128), F32)
    for t in range(BLOCKS):
        src, t0 = (fx, t) if t < X_FIRST else (fy, t - X_FIRST)
        halves = []
        for k in range(2):
            halves.append(
                jnp.concatenate(
                    [src[h, 2 * q + k, i, :, 128 * t0 : 128 * t0 + 128] for h in range(NC) for i in range(NY) for q in range(2)],
                    axis=0,
                )
            )
        d = dot(inverse, jnp.concatenate(halves, axis=1))
        rt_ref[:, 256 * t : 256 * t + 256] = d
        acc = acc + d[:, 0:128] * d[:, 0:128] + d[:, 128:256] * d[:, 128:256]
    sq[z] = jnp.sum(acc.T, axis=0, keepdims=True)
    copies = {}
    for o in offsets(NZ):
        copies[o] = send(sq.at[z], sq.at[z], sq_s.at[o - 1], sq_r.at[o - 1], {"tensor": at_z(o)})
    pending += copies.values()
    for o in range(1, NZ):
        copies[o].wait_recv()
    total = sq[0]
    for i in range(1, NZ):
        total = total + sq[i]
    inv_ref[...] = 1.0 / jnp.sqrt(total / COLS + 1e-06)

    for copy in pending:
        copy.wait_send()


def final_kernel(g_ref, m_ref, rt_ref, ortho_ref, inv_ref, up_ref, nm_ref, nr_ref):
    ortho = ortho_ref[...]
    inv = inv_ref[...]
    rt = rt_ref[...]
    nm_ref[...] = (g_ref[...] + m_ref[...]) - 0.05 * dot(ortho, rt)
    up_ref[...] = dot(ortho * (inv * ((ROWS / RANK) ** 0.5)), rt)
    nr_ref[...] = rt.T * inv


def on_device(gradient, momentum, right_factor):
    vmem = pl.BlockSpec(memory_space=pltpu.VMEM)
    dma = pltpu.SemaphoreType.DMA
    v = lambda *shape: pltpu.VMEM(shape, F32)
    rt, ortho, inv = pl.pallas_call(
        main_kernel,
        name="sums",
        out_shape=(
            jax.ShapeDtypeStruct((RANK, LOCAL_COLS), F32),
            jax.ShapeDtypeStruct((LOCAL_ROWS, RANK), F32),
            jax.ShapeDtypeStruct((1, RANK), F32),
        ),
        in_specs=[vmem] * 3,
        out_specs=[vmem] * 3,
        scratch_shapes=[
            v(128, LOCAL_COLS), v(NZ, 8, RANK), v(NZ - 1, 8, RANK), v(NZ, 8, RANK), v(RANK, 128),
            v(NC, NY, 16, RANK), v(NY, 16, RANK), v(NY - 1, 16, RANK), v(NX, 16, RANK), v(NC, NY, 16, RANK), v(RANK, 2 * RANK),
            v(NC, NX, NY, 8, XW), v(NC, NX, NY, 8, YW), v(NX, NY, 8, XW), v(NX, NY, 8, YW),
            v(NX - 1, NY, 8, XW), v(NY, 8, XW), v(NY - 1, 8, XW),
            v(NY - 1, NX, 8, YW), v(NX, 8, YW), v(NX - 1, 8, YW),
            v(NC, NX, NY, 8, XW), v(NC, NX, NY, 8, YW), v(NZ, 1, RANK),
            dma((NZ - 1,)), dma((NZ - 1,)), dma((NZ - 1,)), dma((NZ - 1,)), dma((3,)), dma((3,)),
            dma((NY - 1,)), dma((NY - 1,)), dma((NX - 1,)), dma((NX - 1,)), dma((NY - 1,)), dma((NY - 1,)), dma, dma,
            dma((NX - 1,)), dma((NX - 1,)), dma((NY - 1,)), dma((NY - 1,)),
            dma((NY - 1,)), dma((NY - 1,)), dma((NX - 1,)), dma((NX - 1,)),
            dma((NY - 1,)), dma((NY - 1,)), dma((NX - 1,)), dma((NX - 1,)),
            dma((NX - 1,)), dma((NX - 1,)), dma((NY - 1,)), dma((NY - 1,)),
            dma((2,)), dma((2,)), dma((NZ - 1,)), dma((NZ - 1,)),
        ],
        compiler_params=pltpu.CompilerParams(
            collective_id=0, has_side_effects=True, vmem_limit_bytes=62 * 2**20
        ),
    )(gradient, momentum, right_factor)
    steps = 3
    width = LOCAL_COLS // steps
    wide = pl.BlockSpec((LOCAL_ROWS, width), lambda i: (0, i))
    return tuple(
        pl.pallas_call(
            final_kernel,
            name="outputs",
            grid=(steps,),
            out_shape=(
                jax.ShapeDtypeStruct((LOCAL_ROWS, LOCAL_COLS), F32),
                jax.ShapeDtypeStruct((LOCAL_ROWS, LOCAL_COLS), F32),
                jax.ShapeDtypeStruct((LOCAL_COLS, RANK), F32),
            ),
            in_specs=[
                wide, wide, pl.BlockSpec((RANK, width), lambda i: (0, i)),
                pl.BlockSpec((LOCAL_ROWS, RANK), lambda i: (0, 0)), pl.BlockSpec((1, RANK), lambda i: (0, 0)),
            ],
            out_specs=[wide, wide, pl.BlockSpec((width, RANK), lambda i: (i, 0))],
        )(gradient, momentum, rt, ortho, inv)
    )


def solution(mesh):
    finer = Mesh(mesh.devices.reshape(NX, NY, NC, mesh.shape["tensor"]), (*DP, "tensor"))
    return jax.shard_map(
        on_device,
        mesh=finer,
        in_specs=(P(DP, "tensor"), P(DP, "tensor"), P("tensor", None)),
        out_specs=(P(DP, "tensor"), P(DP, "tensor"), P("tensor", None)),
        check_vma=False,
    )
```

```python
import jax
import jax.numpy as jnp
from jax import lax
from jax.experimental import pallas as pl
from jax.experimental.pallas import tpu as pltpu
from jax.sharding import Mesh
from jax.sharding import PartitionSpec as P

ROWS = 5120
COLS = 27648
RANK = 256
NX, NY, NC, NZ = 4, 8, 2, 12
DP = ("dp_0", "dp_1", "dp_2")
HIGH = lax.Precision.HIGHEST
F32 = jnp.float32
BF16 = jnp.bfloat16
MESH = pl.DeviceIdType.MESH
LOCAL_ROWS = ROWS // (NX * NY * NC)
LOCAL_COLS = COLS // NZ
CHIP_ROWS = NC * LOCAL_ROWS
LEFT_CHUNKS = LOCAL_ROWS // 8
XS, YB = 3, 3
Y0 = 512 * XS
FETCH = 3
PANEL = 64


def dot(a, b, dims=((1,), (0,))):
    return lax.dot_general(a, b, (dims, ((), ())), precision=HIGH, preferred_element_type=F32)


def eliminate_slab(ws, p, s):
    r0 = PANEL * p + 8 * s
    end = PANEL * (p + 1)
    n = end - r0
    lo = (r0 // 128) * 128
    hi = RANK + (r0 // 128 + 1) * 128
    cols = [jnp.broadcast_to(ws[r0:end, r0 + j : r0 + j + 1], (n, 128)) for j in range(8)]
    w = ws[r0:end, lo:hi]
    sub = lax.broadcasted_iota(jnp.int32, (n, 128), 0)
    wide_sub = lax.broadcasted_iota(jnp.int32, w.shape, 0)
    reps = (hi - lo) // 128
    for j in range(8):
        rs = lax.rsqrt(cols[j][j : j + 1, :])
        l = cols[j] * rs
        for m in range(j + 1, 8):
            cols[m] = cols[m] - l * l[m : m + 1, :]
        lm = jnp.concatenate([jnp.where(sub > j, l, 0.0)] * reps, axis=1)
        u = w[j : j + 1, :] * jnp.concatenate([rs] * reps, axis=1)
        w = jnp.where(wide_sub == j, jnp.broadcast_to(u, w.shape), w - lm * u)
    ws[r0:end, lo:hi] = w


def update_below(ws, p):
    a, b = PANEL * p, PANEL * (p + 1)
    lo = (b // 128) * 128
    hi = RANK + ((b - 1) // 128 + 1) * 128
    full = dot(ws[a:b, lo:RANK], ws[a:b, lo:hi], ((0,), (0,)))
    ws[b:RANK, lo:hi] = ws[b:RANK, lo:hi] - full[b - lo :, :]


def factor_panel(ws, p):
    for s in range(PANEL // 8):
        eliminate_slab(ws, p, s)
    if PANEL * (p + 1) < RANK:
        update_below(ws, p)


def offsets(n):
    return sorted(range(1, n), key=lambda off: -min(off, n - off))


BUFFERS = dict(
    gbuf=(LOCAL_ROWS, LOCAL_COLS),
    mbuf=(LOCAL_ROWS, LOCAL_COLS),
    rfac=(LOCAL_COLS, RANK),
    bb=(CHIP_ROWS, LOCAL_COLS),
    pbuf=(NZ, 8, RANK),
    pin=(NZ - 1, 8, RANK),
    lbuf=(NZ, 8, RANK),
    lpin=(LEFT_CHUNKS, 8, RANK),
    lt=(RANK, CHIP_ROWS),
    gp=(NX, NY, 8, 128),
    gxin=(NX - 1, NY, 8, 128),
    gxs=(NY, 8, 128),
    gyin=(NY - 1, 8, 128),
    gfull=(NC, NX, NY, 8, 128),
    ws=(RANK, 2 * RANK),
    mx=(XS, NX, NY, 16, 128),
    my=(YB, NX, NY, 8, 128),
    x1in=(XS, NX - 1, NY, 16, 128),
    xs=(XS, NY, 16, 128),
    y2in=(XS, NY - 1, 16, 128),
    y1in=(YB, NY - 1, NX, 8, 128),
    ys=(NX, YB, 8, 128),
    x2in=(NX - 1, YB, 8, 128),
    fx=(NC, XS, NX, NY, 16, 128),
    fy=(NC, YB, NX, NY, 8, 128),
    rv=(LOCAL_COLS, RANK),
    sq=(NZ, 1, RANK),
)
REMOTE = dict(
    swap=(2,),
    a1=(NZ - 1,),
    a2=(NZ - 1,),
    g1=(NX - 1,),
    g2=(NY - 1,),
    g3=(NY - 1,),
    g4=(NX - 1,),
    g5=(1,),
    x1=(XS, NX - 1),
    y2=(XS, NY - 1),
    y1=(YB, NY - 1),
    x2=(NX - 1,),
    bx1=(XS, NY - 1),
    bx2=(XS, NX - 1),
    bx3=(XS,),
    by1=(NX - 1,),
    by2=(YB, NY - 1),
    by3=(YB,),
    s1=(NZ - 1,),
)
LOCAL = dict(fetch=(2 + FETCH,), out=(XS + YB,))


def main_kernel(g_ref, m_ref, r_ref, right_ref, ortho_ref, inv_ref, *scratch):
    names = [*BUFFERS, *LOCAL, *(n + e for n in REMOTE for e in ("_send", "_recv"))]
    ref = dict(zip(names, scratch, strict=True))
    gbuf, mbuf, rfac, bb, pbuf, pin, lbuf, lpin, lt = (ref[n] for n in list(BUFFERS)[:9])
    gp, gxin, gxs, gyin, gfull, ws = (ref[n] for n in list(BUFFERS)[9:15])
    mx, my, x1in, xs, y2in, y1in, ys, x2in, fx, fy, rv, sq = (ref[n] for n in list(BUFFERS)[15:])
    x, y, c, z = (lax.axis_index(a) for a in (*DP, "tensor"))
    pair = {"dp_2": 1 - c}
    pending = []

    def at_x(off):
        return lax.rem(x + off, NX)

    def at_y(off):
        return lax.rem(y + off, NY)

    def at_z(off):
        return lax.rem(z + off, NZ)

    def send(name, index, src, dst, where):
        copy = pltpu.make_async_remote_copy(
            src_ref=src,
            dst_ref=dst,
            send_sem=ref[name + "_send"].at[index],
            recv_sem=ref[name + "_recv"].at[index],
            device_id=where,
            device_id_type=MESH,
        )
        copy.start()
        pending.append(copy)
        return copy

    def arrive(copies):
        for copy in copies:
            copy.wait_recv()

    barrier = pltpu.get_barrier_semaphore()
    greet = [{"tensor": at_z(o)} for o in offsets(NZ)]
    greet += [{"dp_1": at_y(o)} for o in offsets(NY)]
    greet += [{"dp_0": at_x(o)} for o in offsets(NX)]
    greet += [pair]
    for where in greet:
        pl.semaphore_signal(barrier, inc=1, device_id=where, device_id_type=MESH)

    depth = LOCAL_COLS // FETCH
    fetches = [(g_ref, gbuf), (m_ref, mbuf)]
    fetches += [(r_ref.at[pl.ds(depth * i, depth)], rfac.at[pl.ds(depth * i, depth)]) for i in range(FETCH)]
    fetches = [pltpu.make_async_copy(src, dst, ref["fetch"].at[i]) for i, (src, dst) in enumerate(fetches)]
    for copy in fetches:
        copy.start()

    fetches[0].wait()
    fetches[1].wait()
    bb[0:LOCAL_ROWS, :] = gbuf[...] + mbuf[...]
    part = None
    for i in range(FETCH):
        fetches[2 + i].wait()
        more = dot(bb[0:LOCAL_ROWS, depth * i : depth * (i + 1)], rfac[depth * i : depth * (i + 1), :])
        part = more if part is None else part + more
    for i in range(NZ):
        pbuf[i] = part[8 * i : 8 * i + 8, :] if i < LEFT_CHUNKS else jnp.zeros((8, RANK), F32)
    pl.semaphore_wait(barrier, len(greet))

    copies = [(o, send("a1", o - 1, pbuf.at[at_z(o)], pin.at[o - 1], {"tensor": at_z(o)})) for o in offsets(NZ)]
    swap_b = send("swap", 0, bb.at[pl.ds(0, LOCAL_ROWS)], bb.at[pl.ds(LOCAL_ROWS, LOCAL_ROWS)], pair)
    total = pbuf[z]
    for o, copy in sorted(copies, key=lambda oc: oc[0]):
        copy.wait_recv()
        total = total + pin[o - 1]
    lbuf[z] = total
    copies = [send("a2", o - 1, lbuf.at[z], lbuf.at[z], {"tensor": at_z(o)}) for o in offsets(NZ)]
    arrive(copies)

    swap_left = send("swap", 1, lbuf.at[pl.ds(0, LEFT_CHUNKS)], lpin, pair)
    swap_left.wait_recv()
    swap_b.wait_recv()
    chip_left = jnp.concatenate([lbuf[i] for i in range(LEFT_CHUNKS)] + [lpin[i] for i in range(LEFT_CHUNKS)], axis=0)
    lt[...] = chip_left.T
    half = lt[pl.ds(pl.multiple_of(128 * c, 128), 128), :]
    gram = dot(half, chip_left)
    for i in range(NX):
        for j in range(NY):
            r0 = 8 * ((i // 2) * NY + j)
            gp[i, j] = gram[r0 : r0 + 8, 128 * (i % 2) : 128 * (i % 2) + 128]
    g1 = {o: send("g1", o - 1, gp.at[at_x(o)], gxin.at[o - 1], {"dp_0": at_x(o)}) for o in offsets(NX)}

    def product(t):
        d = dot(half, bb[:, 256 * t : 256 * t + 256])
        return d[:, 0:128].T, d[:, 128:256].T

    def product_x(s):
        for i in range(2):
            first, second = product(2 * s + i)
            mx[s, 2 * i] = first.reshape(NY, 16, 128)
            mx[s, 2 * i + 1] = second.reshape(NY, 16, 128)
        return {o: send("x1", (s, o - 1), mx.at[s, at_x(o)], x1in.at[s, o - 1], {"dp_0": at_x(o)}) for o in offsets(NX)}

    def product_y(b):
        first, second = product(2 * XS + b)
        my[b, 0:2] = first.reshape(2, NY, 8, 128)
        my[b, 2:4] = second.reshape(2, NY, 8, 128)

    def send_y1(b):
        return {o: send("y1", (b, o - 1), my.at[b, :, at_y(o)], y1in.at[b, o - 1], {"dp_1": at_y(o)}) for o in offsets(NY)}

    y1, x1, y2 = [None] * YB, [None] * XS, [None] * XS
    product_y(0)
    y1[0] = send_y1(0)
    x1[0] = product_x(0)
    product_y(1)
    x1[1] = product_x(1)
    product_y(2)
    x1[2] = product_x(2)

    def sum_x1(s):
        arrive(x1[s].values())
        for i in range(NY):
            acc = mx[s, x, i]
            for o in range(1, NX):
                acc = acc + x1in[s, o - 1, i]
            xs[s, i] = acc
        y2[s] = {o: send("y2", (s, o - 1), xs.at[s, at_y(o)], y2in.at[s, o - 1], {"dp_1": at_y(o)}) for o in offsets(NY)}

    def sum_y1(b):
        arrive(y1[b].values())
        for i in range(NX):
            acc = my[b, i, y]
            for o in range(1, NY):
                acc = acc + y1in[b, o - 1, i]
            ys[i, b] = acc

    arrive(g1.values())
    for j in range(NY):
        acc = gp[x, j]
        for o in range(1, NX):
            acc = acc + gxin[o - 1, j]
        gxs[j] = acc
    g2 = {o: send("g2", o - 1, gxs.at[at_y(o)], gyin.at[o - 1], {"dp_1": at_y(o)}) for o in offsets(NY)}
    y1[1] = send_y1(1)
    sum_x1(0)
    arrive(g2.values())
    acc = gxs[y]
    for o in range(1, NY):
        acc = acc + gyin[o - 1]
    gfull[c, x, y] = acc
    g3 = [send("g3", o - 1, gfull.at[c, x, y], gfull.at[c, x, y], {"dp_1": at_y(o)}) for o in offsets(NY)]
    y1[2] = send_y1(2)
    sum_x1(1)
    sum_y1(0)
    sum_x1(2)
    sum_y1(1)
    arrive(g3)
    g4 = [send("g4", o - 1, gfull.at[c, x], gfull.at[c, x], {"dp_0": at_x(o)}) for o in offsets(NX)]
    sum_y1(2)
    x2 = {o: send("x2", o - 1, ys.at[at_x(o)], x2in.at[o - 1], {"dp_0": at_x(o)}) for o in offsets(NX)}

    def back_x1(s):
        arrive(y2[s].values())
        acc = xs[s, y]
        for o in range(1, NY):
            acc = acc + y2in[s, o - 1]
        fx[c, s, x, y] = acc
        return [send("bx1", (s, o - 1), fx.at[c, s, x, y], fx.at[c, s, x, y], {"dp_1": at_y(o)}) for o in offsets(NY)]

    def back_x2(s):
        arrive(bx1[s])
        return [send("bx2", (s, o - 1), fx.at[c, s, x], fx.at[c, s, x], {"dp_0": at_x(o)}) for o in offsets(NX)]

    def back_x3(s):
        arrive(bx2[s])
        return send("bx3", s, fx.at[c, s], fx.at[c, s], pair)

    bx1, bx2, bx3, by2, by3 = [None] * XS, [None] * XS, [None] * XS, [None] * YB, [None] * YB
    bx1[0] = back_x1(0)
    arrive(g4)
    g5 = send("g5", 0, gfull.at[c], gfull.at[c], pair)
    bx1[1] = back_x1(1)
    bx1[2] = back_x1(2)
    arrive(x2.values())
    acc = ys[x]
    for o in range(1, NX):
        acc = acc + x2in[o - 1]
    fy[c, :, x, y] = acc
    by1 = [send("by1", o - 1, fy.at[c, :, x, y], fy.at[c, :, x, y], {"dp_0": at_x(o)}) for o in offsets(NX)]

    g5.wait_recv()
    for h in range(NC):
        for i in range(NX):
            for j in range(NY):
                r0 = 128 * h + 8 * ((i // 2) * NY + j)
                ws[r0 : r0 + 8, 128 * (i % 2) : 128 * (i % 2) + 128] = gfull[h, i, j]
    ri = lax.broadcasted_iota(jnp.int32, (RANK, RANK), 0)
    ci = lax.broadcasted_iota(jnp.int32, (RANK, RANK), 1)
    ws[:, RANK:] = jnp.where(ri == ci, 1.0, 0.0)

    factor_panel(ws, 0)
    arrive(by1)
    for b in range(YB):
        by2[b] = [
            send("by2", (b, o - 1), fy.at[c, b, :, y], fy.at[c, b, :, y], {"dp_1": at_y(o)}) for o in offsets(NY)
        ]
    factor_panel(ws, 1)
    bx2[0] = back_x2(0)
    factor_panel(ws, 2)
    bx2[1] = back_x2(1)
    factor_panel(ws, 3)
    bx2[2] = back_x2(2)
    inverse = ws[:, RANK:]
    ortho_ref[...] = dot(chip_left[0:LOCAL_ROWS, :], inverse, ((1,), (1,)))

    outs = []

    def right(parts, r0, n):
        d = dot(jnp.concatenate(parts, axis=1), ws[:, RANK:], ((1,), (1,)))
        rv[r0 : r0 + n, :] = d
        copy = pltpu.make_async_copy(rv.at[pl.ds(r0, n)], right_ref.at[pl.ds(r0, n)], ref["out"].at[len(outs)])
        copy.start()
        outs.append(copy)
        return jnp.sum(d * d, axis=0, keepdims=True)

    def right_x(s):
        bx3[s].wait_recv()
        return right([fx[h, s].reshape(512, 128) for h in range(NC)], 512 * s, 512)

    def right_y(b):
        by3[b].wait_recv()
        return right([fy[h, b].reshape(256, 128) for h in range(NC)], Y0 + 256 * b, 256)

    def back_y3(b):
        arrive(by2[b])
        return send("by3", b, fy.at[c, b], fy.at[c, b], pair)

    bx3[0] = back_x3(0)
    by3[0] = back_y3(0)
    squares = right_x(0)
    bx3[1] = back_x3(1)
    by3[1] = back_y3(1)
    squares = squares + right_y(0)
    squares = squares + right_x(1)
    squares = squares + right_y(1)
    bx3[2] = back_x3(2)
    by3[2] = back_y3(2)
    squares = squares + right_x(2)
    squares = squares + right_y(2)

    sq[z] = squares
    copies = [send("s1", o - 1, sq.at[z], sq.at[z], {"tensor": at_z(o)}) for o in offsets(NZ)]
    arrive(copies)
    total = sq[0]
    for i in range(1, NZ):
        total = total + sq[i]
    inv_ref[...] = 1.0 / jnp.sqrt(total / COLS + 1e-06)

    for copy in pending:
        copy.wait_send()
    for copy in outs:
        copy.wait()


def two_parts(a):
    big = a.astype(BF16)
    return big, (a - big.astype(F32)).astype(BF16)


def final_kernel(g_ref, m_ref, r_ref, ortho_ref, inv_ref, up_ref, nm_ref, nr_ref):
    ortho = ortho_ref[...]
    inv = inv_ref[...]
    r = r_ref[...]
    rows = jnp.concatenate([ortho * (inv * ((ROWS / RANK) ** 0.5)), ortho * 0.05], axis=0)
    rows_big, rows_small = two_parts(rows)
    r_big, r_small = two_parts(r)
    dims = (((1,), (1,)), ((), ()))
    both = lax.dot_general(rows_big, r_big, dims, preferred_element_type=F32)
    both = both + lax.dot_general(rows_big, r_small, dims, preferred_element_type=F32)
    both = both + lax.dot_general(rows_small, r_big, dims, preferred_element_type=F32)
    up_ref[...] = both[0:LOCAL_ROWS, :]
    nm_ref[...] = (g_ref[...] + m_ref[...]) - both[LOCAL_ROWS:, :]
    nr_ref[...] = r * inv


def on_device(gradient, momentum, right_factor):
    vmem = pl.BlockSpec(memory_space=pltpu.VMEM)
    hbm = pl.BlockSpec(memory_space=pl.ANY)
    dma = pltpu.SemaphoreType.DMA
    right, ortho, inv = pl.pallas_call(
        main_kernel,
        name="sums",
        out_shape=(
            jax.ShapeDtypeStruct((LOCAL_COLS, RANK), F32),
            jax.ShapeDtypeStruct((LOCAL_ROWS, RANK), F32),
            jax.ShapeDtypeStruct((1, RANK), F32),
        ),
        in_specs=[hbm] * 3,
        out_specs=[hbm, vmem, vmem],
        scratch_shapes=[pltpu.VMEM(shape, F32) for shape in BUFFERS.values()]
        + [dma(shape) for shape in LOCAL.values()]
        + [dma(shape) for shape in REMOTE.values() for _ in range(2)],
        compiler_params=pltpu.CompilerParams(
            collective_id=0, has_side_effects=True, vmem_limit_bytes=62 * 2**20
        ),
    )(gradient, momentum, right_factor)
    steps = 3
    width = LOCAL_COLS // steps
    wide = pl.BlockSpec((LOCAL_ROWS, width), lambda i: (0, i))
    tall = pl.BlockSpec((width, RANK), lambda i: (i, 0))
    return tuple(
        pl.pallas_call(
            final_kernel,
            name="outputs",
            grid=(steps,),
            out_shape=(
                jax.ShapeDtypeStruct((LOCAL_ROWS, LOCAL_COLS), F32),
                jax.ShapeDtypeStruct((LOCAL_ROWS, LOCAL_COLS), F32),
                jax.ShapeDtypeStruct((LOCAL_COLS, RANK), F32),
            ),
            in_specs=[
                wide,
                wide,
                tall,
                pl.BlockSpec((LOCAL_ROWS, RANK), lambda i: (0, 0)),
                pl.BlockSpec((1, RANK), lambda i: (0, 0)),
            ],
            out_specs=[wide, wide, tall],
        )(gradient, momentum, right, ortho, inv)
    )


def solution(mesh):
    finer = Mesh(mesh.devices.reshape(NX, NY, NC, mesh.shape["tensor"]), (*DP, "tensor"))
    return jax.shard_map(
        on_device,
        mesh=finer,
        in_specs=(P(DP, "tensor"), P(DP, "tensor"), P("tensor", None)),
        out_specs=(P(DP, "tensor"), P(DP, "tensor"), P("tensor", None)),
        check_vma=False,
    )
```

```python
import jax
import jax.numpy as jnp
from jax import lax
from jax.experimental import pallas as pl
from jax.experimental.pallas import tpu as pltpu
from jax.sharding import Mesh
from jax.sharding import PartitionSpec as P

ROWS = 5120
COLS = 27648
RANK = 256
NX, NY, NC, NZ = 4, 8, 2, 12
DP = ("dp_0", "dp_1", "dp_2")
HIGH = lax.Precision.HIGHEST
F32 = jnp.float32
BF16 = jnp.bfloat16
MESH = pl.DeviceIdType.MESH
LOCAL_ROWS = ROWS // (NX * NY * NC)
LOCAL_COLS = COLS // NZ
CHIP_ROWS = NC * LOCAL_ROWS
LEFT_CHUNKS = LOCAL_ROWS // 8
XS, YB = 3, 3
Y0 = 512 * XS
FETCH = 3
PANEL = 64
SLAB = 16


def dot(a, b, dims=((1,), (0,))):
    return lax.dot_general(a, b, (dims, ((), ())), precision=HIGH, preferred_element_type=F32)


def eliminate_slab(ws, p, s):
    r0 = PANEL * p + SLAB * s
    end = PANEL * (p + 1)
    n = end - r0
    lo = (r0 // 128) * 128
    hi = RANK + (r0 // 128 + 1) * 128
    cols = [jnp.broadcast_to(ws[r0:end, r0 + j : r0 + j + 1], (n, 128)) for j in range(SLAB)]
    w = ws[r0:end, lo:hi]
    sub = lax.broadcasted_iota(jnp.int32, (n, 128), 0)
    wide_sub = lax.broadcasted_iota(jnp.int32, w.shape, 0)
    reps = (hi - lo) // 128
    for j in range(SLAB):
        rs = lax.rsqrt(cols[j][j : j + 1, :])
        l = cols[j] * rs
        for m in range(j + 1, SLAB):
            cols[m] = cols[m] - l * l[m : m + 1, :]
        lm = jnp.concatenate([jnp.where(sub > j, l, 0.0)] * reps, axis=1)
        u = w[j : j + 1, :] * jnp.concatenate([rs] * reps, axis=1)
        w = jnp.where(wide_sub == j, jnp.broadcast_to(u, w.shape), w - lm * u)
    ws[r0:end, lo:hi] = w


def update_below(ws, p):
    a, b = PANEL * p, PANEL * (p + 1)
    lo = (b // 128) * 128
    hi = RANK + ((b - 1) // 128 + 1) * 128
    full = dot(ws[a:b, lo:RANK], ws[a:b, lo:hi], ((0,), (0,)))
    ws[b:RANK, lo:hi] = ws[b:RANK, lo:hi] - full[b - lo :, :]


def factor_slabs(ws, p, first, last):
    for s in range(first, last):
        eliminate_slab(ws, p, s)


def factor_panel(ws, p):
    factor_slabs(ws, p, 0, PANEL // SLAB)
    if PANEL * (p + 1) < RANK:
        update_below(ws, p)


def offsets(n):
    return sorted(range(1, n), key=lambda off: -min(off, n - off))


BUFFERS = dict(
    gbuf=(LOCAL_ROWS, LOCAL_COLS),
    mbuf=(LOCAL_ROWS, LOCAL_COLS),
    rfac=(LOCAL_COLS, RANK),
    bb=(CHIP_ROWS, LOCAL_COLS),
    pbuf=(NZ, 8, RANK),
    pin=(NZ - 1, 8, RANK),
    lbuf=(NZ, 8, RANK),
    lpin=(LEFT_CHUNKS, 8, RANK),
    lt=(RANK, CHIP_ROWS),
    gp=(NX, NY, 8, 128),
    gxin=(NX - 1, NY, 8, 128),
    gxs=(NY, 8, 128),
    gyin=(NY - 1, 8, 128),
    gfull=(NC, NX, NY, 8, 128),
    ws=(RANK, 2 * RANK),
    mx=(XS, NX, NY, 16, 128),
    my=(YB, NX, NY, 8, 128),
    x1in=(XS, NX - 1, NY, 16, 128),
    xs=(XS, NY, 16, 128),
    y2in=(XS, NY - 1, 16, 128),
    y1in=(YB, NY - 1, NX, 8, 128),
    ys=(NX, YB, 8, 128),
    x2in=(NX - 1, YB, 8, 128),
    fx=(NC, XS, NX, NY, 16, 128),
    fy=(NC, YB, NX, NY, 8, 128),
    rv=(LOCAL_COLS, RANK),
    sq=(NZ, 1, RANK),
    ex=(NC, XS, NY, 16, 128),
    ey=(NC, YB, NX, 8, 128),
    vx=(NX, 1, RANK),
    vy=(NY, 1, RANK),
    tinv=(RANK, RANK),
)
REMOTE = dict(
    swap=(2,),
    a1=(NZ - 1,),
    a2=(NZ - 1,),
    g1=(NX - 1,),
    g2=(NY - 1,),
    g3=(NY - 1,),
    g4=(NX - 1,),
    g5=(1,),
    x1=(XS, NX - 1),
    y2=(XS, NY - 1),
    y1=(YB, NY - 1),
    x2=(NX - 1,),
    bx1=(XS, NY - 1),
    bx2=(XS, NX - 1),
    bx3=(XS,),
    by1=(NX - 1,),
    by2=(YB, NY - 1),
    by3=(YB,),
    s1=(NZ - 1,),
    px=(XS,),
    py=(1,),
    v1=(NX - 1,),
    v2=(NY - 1,),
)
LOCAL = dict(fetch=(3 * FETCH,), out=(XS + YB,))


def main_kernel(g_ref, m_ref, r_ref, right_ref, ortho_ref, inv_ref, *scratch):
    names = [*BUFFERS, *LOCAL, *(n + e for n in REMOTE for e in ("_send", "_recv"))]
    ref = dict(zip(names, scratch, strict=True))
    gbuf, mbuf, rfac, bb, pbuf, pin, lbuf, lpin, lt = (ref[n] for n in list(BUFFERS)[:9])
    gp, gxin, gxs, gyin, gfull, ws = (ref[n] for n in list(BUFFERS)[9:15])
    mx, my, x1in, xs, y2in, y1in, ys, x2in, fx, fy, rv, sq, ex, ey, vx, vy, tinv = (ref[n] for n in list(BUFFERS)[15:])
    x, y, c, z = (lax.axis_index(a) for a in (*DP, "tensor"))
    pair = {"dp_2": 1 - c}
    pending = []

    def at_x(off):
        return lax.rem(x + off, NX)

    def at_y(off):
        return lax.rem(y + off, NY)

    def at_z(off):
        return lax.rem(z + off, NZ)

    def send(name, index, src, dst, where):
        copy = pltpu.make_async_remote_copy(
            src_ref=src,
            dst_ref=dst,
            send_sem=ref[name + "_send"].at[index],
            recv_sem=ref[name + "_recv"].at[index],
            device_id=where,
            device_id_type=MESH,
        )
        copy.start()
        pending.append(copy)
        return copy

    def arrive(copies):
        for copy in copies:
            copy.wait_recv()

    barrier = pltpu.get_barrier_semaphore()
    greet = [{"tensor": at_z(o)} for o in offsets(NZ)]
    greet += [{"dp_1": at_y(o)} for o in offsets(NY)]
    greet += [{"dp_0": at_x(o)} for o in offsets(NX)]
    greet += [pair]
    for where in greet:
        pl.semaphore_signal(barrier, inc=1, device_id=where, device_id_type=MESH)

    depth = LOCAL_COLS // FETCH
    fetches = []
    for i in range(FETCH):
        cols = pl.ds(depth * i, depth)
        for j, (src, dst) in enumerate(
            [
                (g_ref.at[:, cols], gbuf.at[:, cols]),
                (m_ref.at[:, cols], mbuf.at[:, cols]),
                (r_ref.at[cols], rfac.at[cols]),
            ]
        ):
            fetches.append(pltpu.make_async_copy(src, dst, ref["fetch"].at[3 * i + j]))
    for copy in fetches:
        copy.start()

    part = None
    for i in range(FETCH):
        for j in range(3):
            fetches[3 * i + j].wait()
        cols = slice(depth * i, depth * (i + 1))
        bb[0:LOCAL_ROWS, cols] = gbuf[:, cols] + mbuf[:, cols]
        more = dot(bb[0:LOCAL_ROWS, cols], rfac[cols, :])
        part = more if part is None else part + more
    for i in range(NZ):
        pbuf[i] = part[8 * i : 8 * i + 8, :] if i < LEFT_CHUNKS else jnp.zeros((8, RANK), F32)
    pl.semaphore_wait(barrier, len(greet))

    copies = [(o, send("a1", o - 1, pbuf.at[at_z(o)], pin.at[o - 1], {"tensor": at_z(o)})) for o in offsets(NZ)]
    swap_b = send("swap", 0, bb.at[pl.ds(0, LOCAL_ROWS)], bb.at[pl.ds(LOCAL_ROWS, LOCAL_ROWS)], pair)
    total = pbuf[z]
    for o, copy in sorted(copies, key=lambda oc: oc[0]):
        copy.wait_recv()
        total = total + pin[o - 1]
    lbuf[z] = total
    copies = [send("a2", o - 1, lbuf.at[z], lbuf.at[z], {"tensor": at_z(o)}) for o in offsets(NZ)]
    arrive(copies)

    swap_left = send("swap", 1, lbuf.at[pl.ds(0, LEFT_CHUNKS)], lpin, pair)
    swap_left.wait_recv()
    swap_b.wait_recv()
    chip_left = jnp.concatenate([lbuf[i] for i in range(LEFT_CHUNKS)] + [lpin[i] for i in range(LEFT_CHUNKS)], axis=0)
    lt[...] = chip_left.T
    half = lt[pl.ds(pl.multiple_of(128 * c, 128), 128), :]
    gram = dot(half, chip_left)
    for i in range(NX):
        for j in range(NY):
            r0 = 8 * ((i // 2) * NY + j)
            gp[i, j] = gram[r0 : r0 + 8, 128 * (i % 2) : 128 * (i % 2) + 128]
    g1 = {o: send("g1", o - 1, gp.at[at_x(o)], gxin.at[o - 1], {"dp_0": at_x(o)}) for o in offsets(NX)}

    def product(t):
        d = dot(half, bb[:, 256 * t : 256 * t + 256])
        return d[:, 0:128].T, d[:, 128:256].T

    def product_x(s):
        for i in range(2):
            first, second = product(2 * s + i)
            mx[s, 2 * i] = first.reshape(NY, 16, 128)
            mx[s, 2 * i + 1] = second.reshape(NY, 16, 128)
        return {o: send("x1", (s, o - 1), mx.at[s, at_x(o)], x1in.at[s, o - 1], {"dp_0": at_x(o)}) for o in offsets(NX)}

    def product_y(b):
        first, second = product(2 * XS + b)
        my[b, 0:2] = first.reshape(2, NY, 8, 128)
        my[b, 2:4] = second.reshape(2, NY, 8, 128)

    def send_y1(b):
        return {o: send("y1", (b, o - 1), my.at[b, :, at_y(o)], y1in.at[b, o - 1], {"dp_1": at_y(o)}) for o in offsets(NY)}

    y1, x1, y2 = [None] * YB, [None] * XS, [None] * XS
    product_y(0)
    y1[0] = send_y1(0)
    x1[0] = product_x(0)
    product_y(1)
    x1[1] = product_x(1)
    product_y(2)
    x1[2] = product_x(2)

    def sum_x1(s):
        arrive(x1[s].values())
        for i in range(NY):
            acc = mx[s, x, i]
            for o in range(1, NX):
                acc = acc + x1in[s, o - 1, i]
            xs[s, i] = acc
        y2[s] = {o: send("y2", (s, o - 1), xs.at[s, at_y(o)], y2in.at[s, o - 1], {"dp_1": at_y(o)}) for o in offsets(NY)}

    def sum_y1(b):
        arrive(y1[b].values())
        for i in range(NX):
            acc = my[b, i, y]
            for o in range(1, NY):
                acc = acc + y1in[b, o - 1, i]
            ys[i, b] = acc

    arrive(g1.values())
    for j in range(NY):
        acc = gp[x, j]
        for o in range(1, NX):
            acc = acc + gxin[o - 1, j]
        gxs[j] = acc
    g2 = {o: send("g2", o - 1, gxs.at[at_y(o)], gyin.at[o - 1], {"dp_1": at_y(o)}) for o in offsets(NY)}
    y1[1] = send_y1(1)
    sum_x1(0)
    arrive(g2.values())
    acc = gxs[y]
    for o in range(1, NY):
        acc = acc + gyin[o - 1]
    gfull[c, x, y] = acc
    g3 = [send("g3", o - 1, gfull.at[c, x, y], gfull.at[c, x, y], {"dp_1": at_y(o)}) for o in offsets(NY)]
    y1[2] = send_y1(2)
    sum_x1(1)
    sum_y1(0)
    sum_x1(2)
    sum_y1(1)
    arrive(g3)
    g4 = [send("g4", o - 1, gfull.at[c, x], gfull.at[c, x], {"dp_0": at_x(o)}) for o in offsets(NX)]
    sum_y1(2)
    x2 = {o: send("x2", o - 1, ys.at[at_x(o)], x2in.at[o - 1], {"dp_0": at_x(o)}) for o in offsets(NX)}

    def back_x1(s):
        arrive(y2[s].values())
        acc = xs[s, y]
        for o in range(1, NY):
            acc = acc + y2in[s, o - 1]
        fx[c, s, x, y] = acc
        return [send("bx1", (s, o - 1), fx.at[c, s, x, y], fx.at[c, s, x, y], {"dp_1": at_y(o)}) for o in offsets(NY)]

    def back_x2(s):
        arrive(bx1[s])
        px[s] = send("px", s, fx.at[c, s, x], ex.at[c, s], pair)
        ex[c, s] = fx[c, s, x]

    def send_x2(s):
        return [send("bx2", (s, o - 1), fx.at[c, s, x], fx.at[c, s, x], {"dp_0": at_x(o)}) for o in offsets(NX)]

    def back_x3(s):
        arrive(bx2[s])
        return send("bx3", s, fx.at[c, s], fx.at[c, s], pair)

    px, bx1, bx2, bx3, by2, by3 = [None] * XS, [None] * XS, [None] * XS, [None] * XS, [None] * YB, [None] * YB
    bx1[0] = back_x1(0)
    arrive(g4)
    g5 = send("g5", 0, gfull.at[c], gfull.at[c], pair)
    bx1[1] = back_x1(1)
    bx1[2] = back_x1(2)
    arrive(x2.values())
    acc = ys[x]
    for o in range(1, NX):
        acc = acc + x2in[o - 1]
    fy[c, :, x, y] = acc
    by1 = [send("by1", o - 1, fy.at[c, :, x, y], fy.at[c, :, x, y], {"dp_0": at_x(o)}) for o in offsets(NX)]

    g5.wait_recv()
    for h in range(NC):
        for i in range(NX):
            for j in range(NY):
                r0 = 128 * h + 8 * ((i // 2) * NY + j)
                ws[r0 : r0 + 8, 128 * (i % 2) : 128 * (i % 2) + 128] = gfull[h, i, j]
    ri = lax.broadcasted_iota(jnp.int32, (RANK, RANK), 0)
    ci = lax.broadcasted_iota(jnp.int32, (RANK, RANK), 1)
    ws[:, RANK:] = jnp.where(ri == ci, 1.0, 0.0)

    factor_panel(ws, 0)
    back_x2(0)
    bx2[0] = send_x2(0)
    half_panel = PANEL // SLAB // 2
    factor_slabs(ws, 1, 0, half_panel)
    arrive(by1)

    def send_y2(b):
        return [send("by2", (b, o - 1), fy.at[c, b, :, y], fy.at[c, b, :, y], {"dp_1": at_y(o)}) for o in offsets(NY)]

    by2[0] = send_y2(0)
    by2[1] = send_y2(1)
    py = send("py", 0, fy.at[c, :, :, y], ey.at[c], pair)
    ey[c] = fy[c, :, :, y]
    factor_slabs(ws, 1, half_panel, 2 * half_panel)
    update_below(ws, 1)
    back_x2(1)
    bx2[1] = send_x2(1)
    factor_panel(ws, 2)
    back_x2(2)
    factor_panel(ws, 3)
    tinv[...] = ws[:, RANK:].T

    def square_sum(parts):
        d = dot(jnp.concatenate(parts, axis=1), tinv[...])
        return jnp.sum(d * d, axis=0, keepdims=True)

    arrive(px)
    py.wait_recv()
    vx[x] = square_sum([ex[h].reshape(128 * XS, 128) for h in range(NC)])
    v1 = [send("v1", o - 1, vx.at[x], vx.at[x], {"dp_0": at_x(o)}) for o in offsets(NX)]
    bx2[2] = send_x2(2)
    vy[y] = square_sum([ey[h].reshape(8 * NX * YB, 128) for h in range(NC)])
    v2 = [send("v2", o - 1, vy.at[y], vy.at[y], {"dp_1": at_y(o)}) for o in offsets(NY)]
    by2[2] = send_y2(2)
    ortho_ref[...] = dot(chip_left[0:LOCAL_ROWS, :], tinv[...])

    outs = []

    def right(parts, r0, n):
        rv[r0 : r0 + n, :] = dot(jnp.concatenate(parts, axis=1), tinv[...])
        copy = pltpu.make_async_copy(rv.at[pl.ds(r0, n)], right_ref.at[pl.ds(r0, n)], ref["out"].at[len(outs)])
        copy.start()
        outs.append(copy)

    def right_x(s):
        bx3[s].wait_recv()
        right([fx[h, s].reshape(512, 128) for h in range(NC)], 512 * s, 512)

    def right_y(b):
        by3[b].wait_recv()
        right([fy[h, b].reshape(256, 128) for h in range(NC)], Y0 + 256 * b, 256)

    def back_y3(b):
        arrive(by2[b])
        return send("by3", b, fy.at[c, b], fy.at[c, b], pair)

    bx3[0] = back_x3(0)
    by3[0] = back_y3(0)
    right_x(0)
    bx3[1] = back_x3(1)
    right_y(0)
    right_x(1)
    by3[1] = back_y3(1)
    arrive(v1)
    arrive(v2)
    total = vx[0]
    for i in range(1, NX):
        total = total + vx[i]
    for i in range(NY):
        total = total + vy[i]
    sq[z] = total
    s1 = [send("s1", o - 1, sq.at[z], sq.at[z], {"tensor": at_z(o)}) for o in offsets(NZ)]
    bx3[2] = back_x3(2)
    right_y(1)
    by3[2] = back_y3(2)
    right_x(2)
    right_y(2)

    arrive(s1)
    total = sq[0]
    for i in range(1, NZ):
        total = total + sq[i]
    inv_ref[...] = 1.0 / jnp.sqrt(total / COLS + 1e-06)

    for copy in pending:
        copy.wait_send()
    for copy in outs:
        copy.wait()


def two_parts(a):
    big = a.astype(BF16)
    return big, (a - big.astype(F32)).astype(BF16)


def final_kernel(g_ref, m_ref, r_ref, ortho_ref, inv_ref, up_ref, nm_ref, nr_ref):
    ortho = ortho_ref[...]
    inv = inv_ref[...]
    r = r_ref[...]
    rows = jnp.concatenate([ortho * (inv * ((ROWS / RANK) ** 0.5)), ortho * 0.05], axis=0)
    rows_big, rows_small = two_parts(rows)
    r_big, r_small = two_parts(r)
    dims = (((1,), (1,)), ((), ()))
    both = lax.dot_general(rows_big, r_big, dims, preferred_element_type=F32)
    both = both + lax.dot_general(rows_big, r_small, dims, preferred_element_type=F32)
    both = both + lax.dot_general(rows_small, r_big, dims, preferred_element_type=F32)
    up_ref[...] = both[0:LOCAL_ROWS, :]
    nm_ref[...] = (g_ref[...] + m_ref[...]) - both[LOCAL_ROWS:, :]
    nr_ref[...] = r * inv


def on_device(gradient, momentum, right_factor):
    vmem = pl.BlockSpec(memory_space=pltpu.VMEM)
    hbm = pl.BlockSpec(memory_space=pl.ANY)
    dma = pltpu.SemaphoreType.DMA
    right, ortho, inv = pl.pallas_call(
        main_kernel,
        name="sums",
        out_shape=(
            jax.ShapeDtypeStruct((LOCAL_COLS, RANK), F32),
            jax.ShapeDtypeStruct((LOCAL_ROWS, RANK), F32),
            jax.ShapeDtypeStruct((1, RANK), F32),
        ),
        in_specs=[hbm] * 3,
        out_specs=[hbm, vmem, vmem],
        scratch_shapes=[pltpu.VMEM(shape, F32) for shape in BUFFERS.values()]
        + [dma(shape) for shape in LOCAL.values()]
        + [dma(shape) for shape in REMOTE.values() for _ in range(2)],
        compiler_params=pltpu.CompilerParams(
            collective_id=0, has_side_effects=True, vmem_limit_bytes=62 * 2**20
        ),
    )(gradient, momentum, right_factor)
    steps = 2
    width = LOCAL_COLS // steps
    wide = pl.BlockSpec((LOCAL_ROWS, width), lambda i: (0, i))
    tall = pl.BlockSpec((width, RANK), lambda i: (i, 0))
    return tuple(
        pl.pallas_call(
            final_kernel,
            name="outputs",
            grid=(steps,),
            out_shape=(
                jax.ShapeDtypeStruct((LOCAL_ROWS, LOCAL_COLS), F32),
                jax.ShapeDtypeStruct((LOCAL_ROWS, LOCAL_COLS), F32),
                jax.ShapeDtypeStruct((LOCAL_COLS, RANK), F32),
            ),
            in_specs=[
                wide,
                wide,
                tall,
                pl.BlockSpec((LOCAL_ROWS, RANK), lambda i: (0, 0)),
                pl.BlockSpec((1, RANK), lambda i: (0, 0)),
            ],
            out_specs=[wide, wide, tall],
        )(gradient, momentum, right, ortho, inv)
    )


def solution(mesh):
    finer = Mesh(mesh.devices.reshape(NX, NY, NC, mesh.shape["tensor"]), (*DP, "tensor"))
    return jax.shard_map(
        on_device,
        mesh=finer,
        in_specs=(P(DP, "tensor"), P(DP, "tensor"), P("tensor", None)),
        out_specs=(P(DP, "tensor"), P(DP, "tensor"), P("tensor", None)),
        check_vma=False,
    )
```

```python
import jax
import jax.numpy as jnp
from jax import lax
from jax.experimental import pallas as pl
from jax.experimental.pallas import tpu as pltpu
from jax.sharding import Mesh
from jax.sharding import PartitionSpec as P

ROWS = 5120
COLS = 27648
RANK = 256
NX, NY, NC, NZ = 4, 8, 2, 12
DP = ("dp_0", "dp_1", "dp_2")
HIGH = lax.Precision.HIGHEST
F32 = jnp.float32
BF16 = jnp.bfloat16
MESH = pl.DeviceIdType.MESH
LOCAL_ROWS = ROWS // (NX * NY * NC)
LOCAL_COLS = COLS // NZ
CHIP_ROWS = NC * LOCAL_ROWS
LEFT_CHUNKS = LOCAL_ROWS // 8
XS, YB = 3, 3
Y0 = 512 * XS
FETCH = 3
OUT_PARTS = 3
PANEL = 64
SLAB = 16


def dot(a, b, dims=((1,), (0,))):
    return lax.dot_general(a, b, (dims, ((), ())), precision=HIGH, preferred_element_type=F32)


def eliminate_slab(ws, p, s):
    r0 = PANEL * p + SLAB * s
    end = PANEL * (p + 1)
    n = end - r0
    lo = (r0 // 128) * 128
    hi = RANK + (r0 // 128 + 1) * 128
    cols = [jnp.broadcast_to(ws[r0:end, r0 + j : r0 + j + 1], (n, 128)) for j in range(SLAB)]
    w = ws[r0:end, lo:hi]
    sub = lax.broadcasted_iota(jnp.int32, (n, 128), 0)
    wide_sub = lax.broadcasted_iota(jnp.int32, w.shape, 0)
    reps = (hi - lo) // 128
    for j in range(SLAB):
        rs = lax.rsqrt(cols[j][j : j + 1, :])
        l = cols[j] * rs
        for m in range(j + 1, SLAB):
            cols[m] = cols[m] - l * l[m : m + 1, :]
        lm = jnp.concatenate([jnp.where(sub > j, l, 0.0)] * reps, axis=1)
        u = w[j : j + 1, :] * jnp.concatenate([rs] * reps, axis=1)
        w = jnp.where(wide_sub == j, jnp.broadcast_to(u, w.shape), w - lm * u)
    ws[r0:end, lo:hi] = w


def update_below(ws, p):
    a, b = PANEL * p, PANEL * (p + 1)
    lo = (b // 128) * 128
    hi = RANK + ((b - 1) // 128 + 1) * 128
    full = dot(ws[a:b, lo:RANK], ws[a:b, lo:hi], ((0,), (0,)))
    ws[b:RANK, lo:hi] = ws[b:RANK, lo:hi] - full[b - lo :, :]


def factor_slabs(ws, p, first, last):
    for s in range(first, last):
        eliminate_slab(ws, p, s)


def factor_panel(ws, p):
    factor_slabs(ws, p, 0, PANEL // SLAB)
    if PANEL * (p + 1) < RANK:
        update_below(ws, p)


def offsets(n):
    return sorted(range(1, n), key=lambda off: -min(off, n - off))


BUFFERS = dict(
    gbuf=(LOCAL_ROWS, LOCAL_COLS),
    mbuf=(LOCAL_ROWS, LOCAL_COLS),
    rfac=(LOCAL_COLS, RANK),
    bb=(CHIP_ROWS, LOCAL_COLS),
    pbuf=(NZ, 8, RANK),
    pin=(NZ - 1, 8, RANK),
    lbuf=(NZ, 8, RANK),
    lpin=(LEFT_CHUNKS, 8, RANK),
    lt=(RANK, CHIP_ROWS),
    gp=(NX, NY, 8, 128),
    gxin=(NX - 1, NY, 8, 128),
    gxs=(NY, 8, 128),
    gyin=(NY - 1, 8, 128),
    gfull=(NC, NX, NY, 8, 128),
    ws=(RANK, 2 * RANK),
    mx=(XS, NX, NY, 16, 128),
    my=(YB, NX, NY, 8, 128),
    x1in=(XS, NX - 1, NY, 16, 128),
    xs=(XS, NY, 16, 128),
    y2in=(XS, NY - 1, 16, 128),
    y1in=(YB, NY - 1, NX, 8, 128),
    ys=(NX, YB, 8, 128),
    x2in=(NX - 1, YB, 8, 128),
    fx=(NC, XS, NX, NY, 16, 128),
    fy=(NC, YB, NX, NY, 8, 128),
    sq=(NZ, 1, RANK),
    ex=(NC, XS, NY, 16, 128),
    ey=(NC, YB, NX, 8, 128),
    vx=(NX, 1, RANK),
    vy=(NY, 1, RANK),
    tinv=(RANK, RANK),
)
REMOTE = dict(
    swap=(2,),
    a1=(NZ - 1,),
    a2=(NZ - 1,),
    g1=(NX - 1,),
    g2=(NY - 1,),
    g3=(NY - 1,),
    g4=(NX - 1,),
    g5=(1,),
    x1=(XS, NX - 1),
    y2=(XS, NY - 1),
    y1=(YB, NY - 1),
    x2=(NX - 1,),
    bx1=(XS, NY - 1),
    bx2=(XS, NX - 1),
    bx3=(XS,),
    by1=(NX - 1,),
    by2=(YB, NY - 1),
    by3=(YB,),
    s1=(NZ - 1,),
    px=(XS,),
    py=(1,),
    v1=(NX - 1,),
    v2=(NY - 1,),
)
LOCAL = dict(fetch=(3 * FETCH,))


def main_kernel(g_ref, m_ref, r_ref, right_ref, ortho_ref, inv_ref, b_ref, *scratch):
    names = [*BUFFERS, *LOCAL, *(n + e for n in REMOTE for e in ("_send", "_recv"))]
    ref = dict(zip(names, scratch, strict=True))
    gbuf, mbuf, rfac, bb, pbuf, pin, lbuf, lpin, lt = (ref[n] for n in list(BUFFERS)[:9])
    gp, gxin, gxs, gyin, gfull, ws = (ref[n] for n in list(BUFFERS)[9:15])
    mx, my, x1in, xs, y2in, y1in, ys, x2in, fx, fy, sq, ex, ey, vx, vy, tinv = (ref[n] for n in list(BUFFERS)[15:])
    x, y, c, z = (lax.axis_index(a) for a in (*DP, "tensor"))
    pair = {"dp_2": 1 - c}
    pending = []

    def at_x(off):
        return lax.rem(x + off, NX)

    def at_y(off):
        return lax.rem(y + off, NY)

    def at_z(off):
        return lax.rem(z + off, NZ)

    def send(name, index, src, dst, where):
        copy = pltpu.make_async_remote_copy(
            src_ref=src,
            dst_ref=dst,
            send_sem=ref[name + "_send"].at[index],
            recv_sem=ref[name + "_recv"].at[index],
            device_id=where,
            device_id_type=MESH,
        )
        copy.start()
        pending.append(copy)
        return copy

    def arrive(copies):
        for copy in copies:
            copy.wait_recv()

    barrier = pltpu.get_barrier_semaphore()
    greet = [{"tensor": at_z(o)} for o in offsets(NZ)]
    greet += [{"dp_1": at_y(o)} for o in offsets(NY)]
    greet += [{"dp_0": at_x(o)} for o in offsets(NX)]
    greet += [pair]
    for where in greet:
        pl.semaphore_signal(barrier, inc=1, device_id=where, device_id_type=MESH)

    depth = LOCAL_COLS // FETCH
    fetches = []
    for i in range(FETCH):
        cols = pl.ds(depth * i, depth)
        for j, (src, dst) in enumerate(
            [
                (g_ref.at[:, cols], gbuf.at[:, cols]),
                (m_ref.at[:, cols], mbuf.at[:, cols]),
                (r_ref.at[cols], rfac.at[cols]),
            ]
        ):
            fetches.append(pltpu.make_async_copy(src, dst, ref["fetch"].at[3 * i + j]))
    for copy in fetches:
        copy.start()

    part = None
    for i in range(FETCH):
        for j in range(3):
            fetches[3 * i + j].wait()
        cols = slice(depth * i, depth * (i + 1))
        bb[0:LOCAL_ROWS, cols] = gbuf[:, cols] + mbuf[:, cols]
        more = dot(bb[0:LOCAL_ROWS, cols], rfac[cols, :])
        part = more if part is None else part + more
    for i in range(NZ):
        pbuf[i] = part[8 * i : 8 * i + 8, :] if i < LEFT_CHUNKS else jnp.zeros((8, RANK), F32)
    pl.semaphore_wait(barrier, len(greet))

    copies = [(o, send("a1", o - 1, pbuf.at[at_z(o)], pin.at[o - 1], {"tensor": at_z(o)})) for o in offsets(NZ)]
    swap_b = send("swap", 0, bb.at[pl.ds(0, LOCAL_ROWS)], bb.at[pl.ds(LOCAL_ROWS, LOCAL_ROWS)], pair)
    total = pbuf[z]
    for o, copy in sorted(copies, key=lambda oc: oc[0]):
        copy.wait_recv()
        total = total + pin[o - 1]
    lbuf[z] = total
    copies = [send("a2", o - 1, lbuf.at[z], lbuf.at[z], {"tensor": at_z(o)}) for o in offsets(NZ)]
    arrive(copies)

    swap_left = send("swap", 1, lbuf.at[pl.ds(0, LEFT_CHUNKS)], lpin, pair)
    swap_left.wait_recv()
    swap_b.wait_recv()
    chip_left = jnp.concatenate([lbuf[i] for i in range(LEFT_CHUNKS)] + [lpin[i] for i in range(LEFT_CHUNKS)], axis=0)
    lt[...] = chip_left.T
    half = lt[pl.ds(pl.multiple_of(128 * c, 128), 128), :]
    gram = dot(half, chip_left)
    for i in range(NX):
        for j in range(NY):
            r0 = 8 * ((i // 2) * NY + j)
            gp[i, j] = gram[r0 : r0 + 8, 128 * (i % 2) : 128 * (i % 2) + 128]
    g1 = {o: send("g1", o - 1, gp.at[at_x(o)], gxin.at[o - 1], {"dp_0": at_x(o)}) for o in offsets(NX)}

    def product(t):
        d = dot(half, bb[:, 256 * t : 256 * t + 256])
        return d[:, 0:128].T, d[:, 128:256].T

    def product_x(s):
        for i in range(2):
            first, second = product(2 * s + i)
            mx[s, 2 * i] = first.reshape(NY, 16, 128)
            mx[s, 2 * i + 1] = second.reshape(NY, 16, 128)
        return {o: send("x1", (s, o - 1), mx.at[s, at_x(o)], x1in.at[s, o - 1], {"dp_0": at_x(o)}) for o in offsets(NX)}

    def product_y(b):
        first, second = product(2 * XS + b)
        my[b, 0:2] = first.reshape(2, NY, 8, 128)
        my[b, 2:4] = second.reshape(2, NY, 8, 128)

    def send_y1(b):
        return {o: send("y1", (b, o - 1), my.at[b, :, at_y(o)], y1in.at[b, o - 1], {"dp_1": at_y(o)}) for o in offsets(NY)}

    y1, x1, y2 = [None] * YB, [None] * XS, [None] * XS
    product_y(0)
    y1[0] = send_y1(0)
    x1[0] = product_x(0)
    product_y(1)
    x1[1] = product_x(1)
    product_y(2)
    x1[2] = product_x(2)

    def sum_x1(s):
        arrive(x1[s].values())
        for i in range(NY):
            acc = mx[s, x, i]
            for o in range(1, NX):
                acc = acc + x1in[s, o - 1, i]
            xs[s, i] = acc
        y2[s] = {o: send("y2", (s, o - 1), xs.at[s, at_y(o)], y2in.at[s, o - 1], {"dp_1": at_y(o)}) for o in offsets(NY)}

    def sum_y1(b):
        arrive(y1[b].values())
        for i in range(NX):
            acc = my[b, i, y]
            for o in range(1, NY):
                acc = acc + y1in[b, o - 1, i]
            ys[i, b] = acc

    arrive(g1.values())
    for j in range(NY):
        acc = gp[x, j]
        for o in range(1, NX):
            acc = acc + gxin[o - 1, j]
        gxs[j] = acc
    g2 = {o: send("g2", o - 1, gxs.at[at_y(o)], gyin.at[o - 1], {"dp_1": at_y(o)}) for o in offsets(NY)}
    y1[1] = send_y1(1)
    sum_x1(0)
    arrive(g2.values())
    acc = gxs[y]
    for o in range(1, NY):
        acc = acc + gyin[o - 1]
    gfull[c, x, y] = acc
    g3 = [send("g3", o - 1, gfull.at[c, x, y], gfull.at[c, x, y], {"dp_1": at_y(o)}) for o in offsets(NY)]
    y1[2] = send_y1(2)
    sum_x1(1)
    sum_y1(0)
    sum_x1(2)
    sum_y1(1)
    arrive(g3)
    g4 = [send("g4", o - 1, gfull.at[c, x], gfull.at[c, x], {"dp_0": at_x(o)}) for o in offsets(NX)]
    sum_y1(2)
    x2 = {o: send("x2", o - 1, ys.at[at_x(o)], x2in.at[o - 1], {"dp_0": at_x(o)}) for o in offsets(NX)}

    def back_x1(s):
        arrive(y2[s].values())
        acc = xs[s, y]
        for o in range(1, NY):
            acc = acc + y2in[s, o - 1]
        fx[c, s, x, y] = acc
        return [send("bx1", (s, o - 1), fx.at[c, s, x, y], fx.at[c, s, x, y], {"dp_1": at_y(o)}) for o in offsets(NY)]

    def back_x2(s):
        arrive(bx1[s])
        px[s] = send("px", s, fx.at[c, s, x], ex.at[c, s], pair)
        ex[c, s] = fx[c, s, x]

    def send_x2(s):
        return [send("bx2", (s, o - 1), fx.at[c, s, x], fx.at[c, s, x], {"dp_0": at_x(o)}) for o in offsets(NX)]

    def back_x3(s):
        arrive(bx2[s])
        return send("bx3", s, fx.at[c, s], fx.at[c, s], pair)

    px, bx1, bx2, bx3, by2, by3 = [None] * XS, [None] * XS, [None] * XS, [None] * XS, [None] * YB, [None] * YB
    bx1[0] = back_x1(0)
    arrive(g4)
    g5 = send("g5", 0, gfull.at[c], gfull.at[c], pair)
    bx1[1] = back_x1(1)
    g5.wait_recv()
    for h in range(NC):
        for i in range(NX):
            for j in range(NY):
                r0 = 128 * h + 8 * ((i // 2) * NY + j)
                ws[r0 : r0 + 8, 128 * (i % 2) : 128 * (i % 2) + 128] = gfull[h, i, j]
    ri = lax.broadcasted_iota(jnp.int32, (RANK, RANK), 0)
    ci = lax.broadcasted_iota(jnp.int32, (RANK, RANK), 1)
    ws[:, RANK:] = jnp.where(ri == ci, 1.0, 0.0)

    half_panel = PANEL // SLAB // 2
    factor_slabs(ws, 0, 0, 1)
    bx1[2] = back_x1(2)
    arrive(x2.values())
    acc = ys[x]
    for o in range(1, NX):
        acc = acc + x2in[o - 1]
    fy[c, :, x, y] = acc
    by1 = [send("by1", o - 1, fy.at[c, :, x, y], fy.at[c, :, x, y], {"dp_0": at_x(o)}) for o in offsets(NX)]

    factor_slabs(ws, 0, 1, 2 * half_panel)
    update_below(ws, 0)
    back_x2(0)
    bx2[0] = send_x2(0)
    factor_slabs(ws, 1, 0, half_panel)
    factor_slabs(ws, 1, half_panel, 2 * half_panel)
    update_below(ws, 1)
    arrive(by1)

    def send_y2(b):
        return [send("by2", (b, o - 1), fy.at[c, b, :, y], fy.at[c, b, :, y], {"dp_1": at_y(o)}) for o in offsets(NY)]

    by2[0] = send_y2(0)
    by2[1] = send_y2(1)
    py = send("py", 0, fy.at[c, :, :, y], ey.at[c], pair)
    ey[c] = fy[c, :, :, y]
    back_x2(1)
    bx2[1] = send_x2(1)
    factor_panel(ws, 2)
    back_x2(2)
    factor_panel(ws, 3)
    tinv[...] = ws[:, RANK:].T

    def square_sum(parts):
        d = dot(jnp.concatenate(parts, axis=1), tinv[...])
        return jnp.sum(d * d, axis=0, keepdims=True)

    arrive(px)
    py.wait_recv()
    vx[x] = square_sum([ex[h].reshape(128 * XS, 128) for h in range(NC)])
    v1 = [send("v1", o - 1, vx.at[x], vx.at[x], {"dp_0": at_x(o)}) for o in offsets(NX)]
    bx2[2] = send_x2(2)
    vy[y] = square_sum([ey[h].reshape(8 * NX * YB, 128) for h in range(NC)])
    v2 = [send("v2", o - 1, vy.at[y], vy.at[y], {"dp_1": at_y(o)}) for o in offsets(NY)]
    by2[2] = send_y2(2)
    b_ref[...] = bb[0:LOCAL_ROWS, :]
    ortho_ref[...] = dot(chip_left[0:LOCAL_ROWS, :], tinv[...])

    def right(parts, r0, n):
        right_ref[r0 : r0 + n, :] = dot(jnp.concatenate(parts, axis=1), tinv[...])

    def right_x(s):
        bx3[s].wait_recv()
        right([fx[h, s].reshape(512, 128) for h in range(NC)], 512 * s, 512)

    def right_y(b):
        by3[b].wait_recv()
        right([fy[h, b].reshape(256, 128) for h in range(NC)], Y0 + 256 * b, 256)

    def back_y3(b):
        arrive(by2[b])
        return send("by3", b, fy.at[c, b], fy.at[c, b], pair)

    bx3[0] = back_x3(0)
    by3[0] = back_y3(0)
    right_x(0)
    bx3[1] = back_x3(1)
    right_y(0)
    arrive(v1)
    arrive(v2)
    total = vx[0]
    for i in range(1, NX):
        total = total + vx[i]
    for i in range(NY):
        total = total + vy[i]
    sq[z] = total
    s1 = [send("s1", o - 1, sq.at[z], sq.at[z], {"tensor": at_z(o)}) for o in offsets(NZ)]
    by3[1] = back_y3(1)
    right_x(1)
    bx3[2] = back_x3(2)
    right_y(1)
    by3[2] = back_y3(2)
    right_x(2)
    right_y(2)

    arrive(s1)
    total = sq[0]
    for i in range(1, NZ):
        total = total + sq[i]
    inv_ref[...] = 1.0 / jnp.sqrt(total / COLS + 1e-06)

    for copy in pending:
        copy.wait_send()


def two_parts(a):
    big = a.astype(BF16)
    return big, (a - big.astype(F32)).astype(BF16)


def final_kernel(b_ref, r_ref, ortho_ref, inv_ref, up_ref, nm_ref, nr_ref, up, nm, nr, sems):
    ortho = ortho_ref[...]
    inv = inv_ref[...]
    rows = jnp.concatenate([ortho * (inv * ((ROWS / RANK) ** 0.5)), ortho * 0.05], axis=0)
    rows_big, rows_small = two_parts(rows)
    dims = (((1,), (1,)), ((), ()))
    copies = []

    def put(src, dst):
        copy = pltpu.make_async_copy(src, dst, sems.at[len(copies)])
        copy.start()
        copies.append(copy)

    width = LOCAL_COLS // OUT_PARTS
    for i in range(OUT_PARTS):
        span = slice(width * i, width * (i + 1))
        here = pl.ds(width * i, width)
        r = r_ref[span, :]
        nr[span, :] = r * inv
        put(nr.at[here], nr_ref.at[here])
        r_big, r_small = two_parts(r)
        both = lax.dot_general(rows_big, r_big, dims, preferred_element_type=F32)
        both = both + lax.dot_general(rows_big, r_small, dims, preferred_element_type=F32)
        both = both + lax.dot_general(rows_small, r_big, dims, preferred_element_type=F32)
        up[:, span] = both[0:LOCAL_ROWS, :]
        put(up.at[:, here], up_ref.at[:, here])
        nm[:, span] = b_ref[:, span] - both[LOCAL_ROWS:, :]
        put(nm.at[:, here], nm_ref.at[:, here])
    for copy in copies:
        copy.wait()


def on_device(gradient, momentum, right_factor):
    vmem = pl.BlockSpec(memory_space=pltpu.VMEM)
    hbm = pl.BlockSpec(memory_space=pltpu.HBM)
    dma = pltpu.SemaphoreType.DMA
    shape = lambda *lengths: jax.ShapeDtypeStruct(lengths, F32)
    right, ortho, inv, buffer = pl.pallas_call(
        main_kernel,
        name="sums",
        out_shape=(
            pltpu.VMEM((LOCAL_COLS, RANK), F32),
            pltpu.VMEM((LOCAL_ROWS, RANK), F32),
            pltpu.VMEM((1, RANK), F32),
            pltpu.VMEM((LOCAL_ROWS, LOCAL_COLS), F32),
        ),
        in_specs=[hbm] * 3,
        out_specs=[vmem] * 4,
        scratch_shapes=[pltpu.VMEM(lengths, F32) for lengths in BUFFERS.values()]
        + [dma(lengths) for lengths in LOCAL.values()]
        + [dma(lengths) for lengths in REMOTE.values() for _ in range(2)],
        compiler_params=pltpu.CompilerParams(
            collective_id=0, has_side_effects=True, vmem_limit_bytes=59_000_000
        ),
    )(gradient, momentum, right_factor)
    outs = (shape(LOCAL_ROWS, LOCAL_COLS), shape(LOCAL_ROWS, LOCAL_COLS), shape(LOCAL_COLS, RANK))
    return tuple(
        pl.pallas_call(
            final_kernel,
            name="outputs",
            out_shape=outs,
            in_specs=[vmem] * 4,
            out_specs=[hbm] * 3,
            scratch_shapes=[pltpu.VMEM(out.shape, F32) for out in outs] + [dma((3 * OUT_PARTS,))],
            compiler_params=pltpu.CompilerParams(vmem_limit_bytes=24 * 2**20),
        )(buffer, right, ortho, inv)
    )


def solution(mesh):
    finer = Mesh(mesh.devices.reshape(NX, NY, NC, mesh.shape["tensor"]), (*DP, "tensor"))
    return jax.shard_map(
        on_device,
        mesh=finer,
        in_specs=(P(DP, "tensor"), P(DP, "tensor"), P("tensor", None)),
        out_specs=(P(DP, "tensor"), P(DP, "tensor"), P("tensor", None)),
        check_vma=False,
    )
```

```python
import jax
import jax.numpy as jnp
from jax import lax
from jax.experimental import pallas as pl
from jax.experimental.pallas import tpu as pltpu
from jax.sharding import Mesh
from jax.sharding import PartitionSpec as P

ROWS = 5120
COLS = 27648
RANK = 256
NX, NY, NC, NZ = 4, 8, 2, 12
DP = ("dp_0", "dp_1", "dp_2")
HIGH = lax.Precision.HIGHEST
F32 = jnp.float32
BF16 = jnp.bfloat16
MESH = pl.DeviceIdType.MESH
LOCAL_ROWS = ROWS // (NX * NY * NC)
LOCAL_COLS = COLS // NZ
CHIP_ROWS = NC * LOCAL_ROWS
LEFT_CHUNKS = LOCAL_ROWS // 8
XS, YB = 3, 3
Y0 = 512 * XS
FETCH = 3
OUT_PARTS = 3
PANEL = 64
SLAB = 16


def dot(a, b, dims=((1,), (0,))):
    return lax.dot_general(a, b, (dims, ((), ())), precision=HIGH, preferred_element_type=F32)


def eliminate_slab(ws, p, s):
    r0 = PANEL * p + SLAB * s
    end = PANEL * (p + 1)
    n = end - r0
    lo = (r0 // 128) * 128
    hi = RANK + (r0 // 128 + 1) * 128
    cols = [jnp.broadcast_to(ws[r0:end, r0 + j : r0 + j + 1], (n, 128)) for j in range(SLAB)]
    w = ws[r0:end, lo:hi]
    sub = lax.broadcasted_iota(jnp.int32, (n, 128), 0)
    wide_sub = lax.broadcasted_iota(jnp.int32, w.shape, 0)
    reps = (hi - lo) // 128
    for j in range(SLAB):
        rs = lax.rsqrt(cols[j][j : j + 1, :])
        l = cols[j] * rs
        for m in range(j + 1, SLAB):
            cols[m] = cols[m] - l * l[m : m + 1, :]
        lm = jnp.concatenate([jnp.where(sub > j, l, 0.0)] * reps, axis=1)
        u = w[j : j + 1, :] * jnp.concatenate([rs] * reps, axis=1)
        w = jnp.where(wide_sub == j, jnp.broadcast_to(u, w.shape), w - lm * u)
    ws[r0:end, lo:hi] = w


def update_below(ws, p):
    a, b = PANEL * p, PANEL * (p + 1)
    lo = (b // 128) * 128
    hi = RANK + ((b - 1) // 128 + 1) * 128
    full = dot(ws[a:b, lo:RANK], ws[a:b, lo:hi], ((0,), (0,)))
    ws[b:RANK, lo:hi] = ws[b:RANK, lo:hi] - full[b - lo :, :]


def factor_slabs(ws, p, first, last):
    for s in range(first, last):
        eliminate_slab(ws, p, s)


def factor_panel(ws, p):
    factor_slabs(ws, p, 0, PANEL // SLAB)
    if PANEL * (p + 1) < RANK:
        update_below(ws, p)


def offsets(n):
    return sorted(range(1, n), key=lambda off: -min(off, n - off))


BUFFERS = dict(
    gbuf=(LOCAL_ROWS, LOCAL_COLS),
    mbuf=(LOCAL_ROWS, LOCAL_COLS),
    rfac=(LOCAL_COLS, RANK),
    bb=(CHIP_ROWS, LOCAL_COLS),
    pbuf=(NZ, 8, RANK),
    pin=(NZ - 1, 8, RANK),
    lbuf=(NZ, 8, RANK),
    lpin=(LEFT_CHUNKS, 8, RANK),
    lt=(RANK, CHIP_ROWS),
    gp=(NX, NY, 8, 128),
    gxin=(NX - 1, NY, 8, 128),
    gxs=(NY, 8, 128),
    gyin=(NY - 1, 8, 128),
    gfull=(NC, NX, NY, 8, 128),
    ws=(RANK, 2 * RANK),
    mx=(XS, NX, NY, 16, 128),
    my=(YB, NX, NY, 8, 128),
    x1in=(XS, NX - 1, NY, 16, 128),
    xs=(XS, NY, 16, 128),
    y2in=(XS, NY - 1, 16, 128),
    y1in=(YB, NY - 1, NX, 8, 128),
    ys=(NX, YB, 8, 128),
    x2in=(NX - 1, YB, 8, 128),
    fx=(NC, XS, NX, NY, 16, 128),
    fy=(NC, YB, NX, NY, 8, 128),
    sq=(NZ, 1, RANK),
    ex=(NC, XS, NY, 16, 128),
    ey=(NC, YB, NX, 8, 128),
    vx=(NX, 1, RANK),
    vy=(NY, 1, RANK),
    tinv=(RANK, RANK),
)
REMOTE = dict(
    swap=(2,),
    a1=(NZ - 1,),
    a2=(NZ - 1,),
    g1=(NX - 1,),
    g2=(NY - 1,),
    g3=(NY - 1,),
    g4=(NX - 1,),
    g5=(1,),
    x1=(XS, NX - 1),
    y2=(XS, NY - 1),
    y1=(YB, NY - 1),
    x2=(NX - 1,),
    bx1=(XS, NY - 1),
    bx2=(XS, NX - 1),
    bx3=(XS,),
    by1=(NX - 1,),
    by2=(YB, NY - 1),
    by3=(YB,),
    s1=(NZ - 1,),
    px=(XS,),
    py=(1,),
    v1=(NX - 1,),
    v2=(NY - 1,),
)
LOCAL = dict(fetch=(3 * FETCH,))


def main_kernel(g_ref, m_ref, r_ref, right_ref, ortho_ref, inv_ref, b_ref, *scratch):
    names = [*BUFFERS, *LOCAL, *(n + e for n in REMOTE for e in ("_send", "_recv"))]
    ref = dict(zip(names, scratch, strict=True))
    gbuf, mbuf, rfac, bb, pbuf, pin, lbuf, lpin, lt = (ref[n] for n in list(BUFFERS)[:9])
    gp, gxin, gxs, gyin, gfull, ws = (ref[n] for n in list(BUFFERS)[9:15])
    mx, my, x1in, xs, y2in, y1in, ys, x2in, fx, fy, sq, ex, ey, vx, vy, tinv = (ref[n] for n in list(BUFFERS)[15:])
    x, y, c, z = (lax.axis_index(a) for a in (*DP, "tensor"))
    pair = {"dp_2": 1 - c}
    pending = []

    def at_x(off):
        return lax.rem(x + off, NX)

    def at_y(off):
        return lax.rem(y + off, NY)

    def at_z(off):
        return lax.rem(z + off, NZ)

    def send(name, index, src, dst, where):
        copy = pltpu.make_async_remote_copy(
            src_ref=src,
            dst_ref=dst,
            send_sem=ref[name + "_send"].at[index],
            recv_sem=ref[name + "_recv"].at[index],
            device_id=where,
            device_id_type=MESH,
        )
        copy.start()
        pending.append(copy)
        return copy

    def arrive(copies):
        for copy in copies:
            copy.wait_recv()

    depth = LOCAL_COLS // FETCH
    fetches = []
    for i in range(FETCH):
        cols = pl.ds(depth * i, depth)
        for j, (src, dst) in enumerate(
            [
                (g_ref.at[:, cols], gbuf.at[:, cols]),
                (m_ref.at[:, cols], mbuf.at[:, cols]),
                (r_ref.at[cols], rfac.at[cols]),
            ]
        ):
            fetches.append(pltpu.make_async_copy(src, dst, ref["fetch"].at[3 * i + j]))
    for copy in fetches:
        copy.start()

    barrier = pltpu.get_barrier_semaphore()
    greet = [{"tensor": at_z(o)} for o in offsets(NZ)]
    greet += [{"dp_1": at_y(o)} for o in offsets(NY)]
    greet += [{"dp_0": at_x(o)} for o in offsets(NX)]
    greet += [pair]
    for where in greet:
        pl.semaphore_signal(barrier, inc=1, device_id=where, device_id_type=MESH)

    part = None
    for i in range(FETCH):
        for j in range(3):
            fetches[3 * i + j].wait()
        cols = slice(depth * i, depth * (i + 1))
        bb[0:LOCAL_ROWS, cols] = gbuf[:, cols] + mbuf[:, cols]
        more = dot(bb[0:LOCAL_ROWS, cols], rfac[cols, :])
        part = more if part is None else part + more
    for i in range(NZ):
        pbuf[i] = part[8 * i : 8 * i + 8, :] if i < LEFT_CHUNKS else jnp.zeros((8, RANK), F32)
    pl.semaphore_wait(barrier, len(greet))

    copies = [(o, send("a1", o - 1, pbuf.at[at_z(o)], pin.at[o - 1], {"tensor": at_z(o)})) for o in offsets(NZ)]
    swap_b = send("swap", 0, bb.at[pl.ds(0, LOCAL_ROWS)], bb.at[pl.ds(LOCAL_ROWS, LOCAL_ROWS)], pair)
    total = pbuf[z]
    for o, copy in sorted(copies, key=lambda oc: oc[0]):
        copy.wait_recv()
        total = total + pin[o - 1]
    lbuf[z] = total
    copies = [send("a2", o - 1, lbuf.at[z], lbuf.at[z], {"tensor": at_z(o)}) for o in offsets(NZ)]
    arrive(copies)

    swap_left = send("swap", 1, lbuf.at[pl.ds(0, LEFT_CHUNKS)], lpin, pair)
    swap_left.wait_recv()
    swap_b.wait_recv()
    chip_left = jnp.concatenate([lbuf[i] for i in range(LEFT_CHUNKS)] + [lpin[i] for i in range(LEFT_CHUNKS)], axis=0)
    lt[...] = chip_left.T
    half = lt[pl.ds(pl.multiple_of(128 * c, 128), 128), :]
    gram = dot(half, chip_left)
    for i in range(NX):
        for j in range(NY):
            r0 = 8 * ((i // 2) * NY + j)
            gp[i, j] = gram[r0 : r0 + 8, 128 * (i % 2) : 128 * (i % 2) + 128]
    g1 = {o: send("g1", o - 1, gp.at[at_x(o)], gxin.at[o - 1], {"dp_0": at_x(o)}) for o in offsets(NX)}

    def product(t):
        d = dot(half, bb[:, 256 * t : 256 * t + 256])
        return d[:, 0:128].T, d[:, 128:256].T

    def product_x(s):
        for i in range(2):
            first, second = product(2 * s + i)
            mx[s, 2 * i] = first.reshape(NY, 16, 128)
            mx[s, 2 * i + 1] = second.reshape(NY, 16, 128)
        return {o: send("x1", (s, o - 1), mx.at[s, at_x(o)], x1in.at[s, o - 1], {"dp_0": at_x(o)}) for o in offsets(NX)}

    def product_y(b):
        first, second = product(2 * XS + b)
        my[b, 0:2] = first.reshape(2, NY, 8, 128)
        my[b, 2:4] = second.reshape(2, NY, 8, 128)

    def send_y1(b):
        return {o: send("y1", (b, o - 1), my.at[b, :, at_y(o)], y1in.at[b, o - 1], {"dp_1": at_y(o)}) for o in offsets(NY)}

    y1, x1, y2 = [None] * YB, [None] * XS, [None] * XS
    product_y(0)
    y1[0] = send_y1(0)
    x1[0] = product_x(0)
    product_y(1)
    x1[1] = product_x(1)
    product_y(2)
    x1[2] = product_x(2)

    def sum_x1(s):
        arrive(x1[s].values())
        for i in range(NY):
            acc = mx[s, x, i]
            for o in range(1, NX):
                acc = acc + x1in[s, o - 1, i]
            xs[s, i] = acc
        y2[s] = {o: send("y2", (s, o - 1), xs.at[s, at_y(o)], y2in.at[s, o - 1], {"dp_1": at_y(o)}) for o in offsets(NY)}

    def sum_y1(b):
        arrive(y1[b].values())
        for i in range(NX):
            acc = my[b, i, y]
            for o in range(1, NY):
                acc = acc + y1in[b, o - 1, i]
            ys[i, b] = acc

    arrive(g1.values())
    for j in range(NY):
        acc = gp[x, j]
        for o in range(1, NX):
            acc = acc + gxin[o - 1, j]
        gxs[j] = acc
    g2 = {o: send("g2", o - 1, gxs.at[at_y(o)], gyin.at[o - 1], {"dp_1": at_y(o)}) for o in offsets(NY)}
    y1[1] = send_y1(1)
    sum_x1(0)
    arrive(g2.values())
    acc = gxs[y]
    for o in range(1, NY):
        acc = acc + gyin[o - 1]
    gfull[c, x, y] = acc
    g3 = [send("g3", o - 1, gfull.at[c, x, y], gfull.at[c, x, y], {"dp_1": at_y(o)}) for o in offsets(NY)]
    y1[2] = send_y1(2)
    sum_x1(1)
    sum_y1(0)
    sum_x1(2)
    sum_y1(1)
    arrive(g3)
    g4 = [send("g4", o - 1, gfull.at[c, x], gfull.at[c, x], {"dp_0": at_x(o)}) for o in offsets(NX)]
    sum_y1(2)
    x2 = {o: send("x2", o - 1, ys.at[at_x(o)], x2in.at[o - 1], {"dp_0": at_x(o)}) for o in offsets(NX)}

    def back_x1(s):
        arrive(y2[s].values())
        acc = xs[s, y]
        for o in range(1, NY):
            acc = acc + y2in[s, o - 1]
        fx[c, s, x, y] = acc
        return [send("bx1", (s, o - 1), fx.at[c, s, x, y], fx.at[c, s, x, y], {"dp_1": at_y(o)}) for o in offsets(NY)]

    def back_x2(s):
        arrive(bx1[s])
        px[s] = send("px", s, fx.at[c, s, x], ex.at[c, s], pair)
        ex[c, s] = fx[c, s, x]

    def send_x2(s):
        return [send("bx2", (s, o - 1), fx.at[c, s, x], fx.at[c, s, x], {"dp_0": at_x(o)}) for o in offsets(NX)]

    def back_x3(s):
        arrive(bx2[s])
        return send("bx3", s, fx.at[c, s], fx.at[c, s], pair)

    px, bx1, bx2, bx3, by2, by3 = [None] * XS, [None] * XS, [None] * XS, [None] * XS, [None] * YB, [None] * YB
    bx1[0] = back_x1(0)
    arrive(g4)
    g5 = send("g5", 0, gfull.at[c], gfull.at[c], pair)
    bx1[1] = back_x1(1)
    g5.wait_recv()
    for h in range(NC):
        for i in range(NX):
            for j in range(NY):
                r0 = 128 * h + 8 * ((i // 2) * NY + j)
                ws[r0 : r0 + 8, 128 * (i % 2) : 128 * (i % 2) + 128] = gfull[h, i, j]
    ri = lax.broadcasted_iota(jnp.int32, (RANK, RANK), 0)
    ci = lax.broadcasted_iota(jnp.int32, (RANK, RANK), 1)
    ws[:, RANK:] = jnp.where(ri == ci, 1.0, 0.0)

    half_panel = PANEL // SLAB // 2
    factor_slabs(ws, 0, 0, 1)
    bx1[2] = back_x1(2)
    arrive(x2.values())
    acc = ys[x]
    for o in range(1, NX):
        acc = acc + x2in[o - 1]
    fy[c, :, x, y] = acc
    by1 = [send("by1", o - 1, fy.at[c, :, x, y], fy.at[c, :, x, y], {"dp_0": at_x(o)}) for o in offsets(NX)]

    factor_slabs(ws, 0, 1, 2 * half_panel)
    update_below(ws, 0)
    back_x2(0)
    bx2[0] = send_x2(0)
    factor_slabs(ws, 1, 0, half_panel)
    factor_slabs(ws, 1, half_panel, 2 * half_panel)
    update_below(ws, 1)
    arrive(by1)

    def send_y2(b):
        return [send("by2", (b, o - 1), fy.at[c, b, :, y], fy.at[c, b, :, y], {"dp_1": at_y(o)}) for o in offsets(NY)]

    by2[0] = send_y2(0)
    by2[1] = send_y2(1)
    py = send("py", 0, fy.at[c, :, :, y], ey.at[c], pair)
    ey[c] = fy[c, :, :, y]
    back_x2(1)
    bx2[1] = send_x2(1)
    factor_panel(ws, 2)
    back_x2(2)
    factor_panel(ws, 3)
    tinv[...] = ws[:, RANK:].T

    def square_sum(parts):
        d = dot(jnp.concatenate(parts, axis=1), tinv[...])
        return jnp.sum(d * d, axis=0, keepdims=True)

    arrive(px)
    py.wait_recv()
    vx[x] = square_sum([ex[h].reshape(128 * XS, 128) for h in range(NC)])
    v1 = [send("v1", o - 1, vx.at[x], vx.at[x], {"dp_0": at_x(o)}) for o in offsets(NX)]
    bx2[2] = send_x2(2)
    vy[y] = square_sum([ey[h].reshape(8 * NX * YB, 128) for h in range(NC)])
    v2 = [send("v2", o - 1, vy.at[y], vy.at[y], {"dp_1": at_y(o)}) for o in offsets(NY)]
    by2[2] = send_y2(2)
    b_ref[...] = bb[0:LOCAL_ROWS, :]
    ortho_ref[...] = dot(chip_left[0:LOCAL_ROWS, :], tinv[...])

    def right(parts, r0, n):
        right_ref[r0 : r0 + n, :] = dot(jnp.concatenate(parts, axis=1), tinv[...])

    def right_x(s):
        bx3[s].wait_recv()
        right([fx[h, s].reshape(512, 128) for h in range(NC)], 512 * s, 512)

    def right_y(b):
        by3[b].wait_recv()
        right([fy[h, b].reshape(256, 128) for h in range(NC)], Y0 + 256 * b, 256)

    def back_y3(b):
        arrive(by2[b])
        return send("by3", b, fy.at[c, b], fy.at[c, b], pair)

    bx3[0] = back_x3(0)
    by3[0] = back_y3(0)
    right_x(0)
    bx3[1] = back_x3(1)
    right_y(0)
    arrive(v1)
    arrive(v2)
    total = vx[0]
    for i in range(1, NX):
        total = total + vx[i]
    for i in range(NY):
        total = total + vy[i]
    sq[z] = total
    s1 = [send("s1", o - 1, sq.at[z], sq.at[z], {"tensor": at_z(o)}) for o in offsets(NZ)]
    by3[1] = back_y3(1)
    right_x(1)
    bx3[2] = back_x3(2)
    right_y(1)
    by3[2] = back_y3(2)
    right_x(2)
    right_y(2)

    arrive(s1)
    total = sq[0]
    for i in range(1, NZ):
        total = total + sq[i]
    inv_ref[...] = 1.0 / jnp.sqrt(total / COLS + 1e-06)

    for copy in pending:
        copy.wait_send()


def two_parts(a):
    big = a.astype(BF16)
    return big, (a - big.astype(F32)).astype(BF16)


def final_kernel(b_ref, r_ref, ortho_ref, inv_ref, up_ref, nm_ref, nr_ref, up, nm, nr, sems):
    ortho = ortho_ref[...]
    inv = inv_ref[...]
    rows = jnp.concatenate([ortho * (inv * ((ROWS / RANK) ** 0.5)), ortho * 0.05], axis=0)
    rows_big, rows_small = two_parts(rows)
    dims = (((1,), (1,)), ((), ()))
    copies = []

    def put(src, dst):
        copy = pltpu.make_async_copy(src, dst, sems.at[len(copies)])
        copy.start()
        copies.append(copy)

    width = LOCAL_COLS // OUT_PARTS
    for i in range(OUT_PARTS):
        span = slice(width * i, width * (i + 1))
        here = pl.ds(width * i, width)
        r = r_ref[span, :]
        nr[span, :] = r * inv
        put(nr.at[here], nr_ref.at[here])
        r_big, r_small = two_parts(r)
        both = lax.dot_general(rows_big, r_big, dims, preferred_element_type=F32)
        both = both + lax.dot_general(rows_big, r_small, dims, preferred_element_type=F32)
        both = both + lax.dot_general(rows_small, r_big, dims, preferred_element_type=F32)
        up[:, span] = both[0:LOCAL_ROWS, :]
        put(up.at[:, here], up_ref.at[:, here])
        nm[:, span] = b_ref[:, span] - both[LOCAL_ROWS:, :]
        put(nm.at[:, here], nm_ref.at[:, here])
    for copy in copies:
        copy.wait()


def on_device(gradient, momentum, right_factor):
    vmem = pl.BlockSpec(memory_space=pltpu.VMEM)
    hbm = pl.BlockSpec(memory_space=pltpu.HBM)
    dma = pltpu.SemaphoreType.DMA
    shape = lambda *lengths: jax.ShapeDtypeStruct(lengths, F32)
    right, ortho, inv, buffer = pl.pallas_call(
        main_kernel,
        name="sums",
        out_shape=(
            pltpu.VMEM((LOCAL_COLS, RANK), F32),
            pltpu.VMEM((LOCAL_ROWS, RANK), F32),
            pltpu.VMEM((1, RANK), F32),
            pltpu.VMEM((LOCAL_ROWS, LOCAL_COLS), F32),
        ),
        in_specs=[hbm] * 3,
        out_specs=[vmem] * 4,
        scratch_shapes=[pltpu.VMEM(lengths, F32) for lengths in BUFFERS.values()]
        + [dma(lengths) for lengths in LOCAL.values()]
        + [dma(lengths) for lengths in REMOTE.values() for _ in range(2)],
        compiler_params=pltpu.CompilerParams(
            collective_id=0, has_side_effects=True, vmem_limit_bytes=59_000_000
        ),
    )(gradient, momentum, right_factor)
    outs = (shape(LOCAL_ROWS, LOCAL_COLS), shape(LOCAL_ROWS, LOCAL_COLS), shape(LOCAL_COLS, RANK))
    return tuple(
        pl.pallas_call(
            final_kernel,
            name="outputs",
            out_shape=outs,
            in_specs=[vmem] * 4,
            out_specs=[hbm] * 3,
            scratch_shapes=[pltpu.VMEM(out.shape, F32) for out in outs] + [dma((3 * OUT_PARTS,))],
            compiler_params=pltpu.CompilerParams(vmem_limit_bytes=24 * 2**20),
        )(buffer, right, ortho, inv)
    )


def solution(mesh):
    finer = Mesh(mesh.devices.reshape(NX, NY, NC, mesh.shape["tensor"]), (*DP, "tensor"))
    return jax.shard_map(
        on_device,
        mesh=finer,
        in_specs=(P(DP, "tensor"), P(DP, "tensor"), P("tensor", None)),
        out_specs=(P(DP, "tensor"), P(DP, "tensor"), P("tensor", None)),
        check_vma=False,
    )
```
